256 devices in a mesh: dom: 64 (over z, x, core), rep: 4 (over y).
Axes of the slice: x: 4, y: 4, z: 8, core: 2. Of those that a mesh axis runs over, the one named last changes fastest.
Arguments:
- features: bfloat16 [524288, 128], P('dom'), may hold values from -6 to 6
- weight: bfloat16 [128, 256], replicated, may hold values from -0.5 to 0.5
- out_grad: bfloat16 [524288, 256], P(('dom', 'rep')), may hold values from -6 to 6
- send_rows: int32 [64, 64, 64], P('dom'), may hold values from 0 to 8191, as said below
- send_count: int32 [64, 64], P('dom'), may hold values from 0 to 64, as said below
- tile_target: int32 [64, 4, 256], P('dom', 'rep'), may hold values from 0 to 15, as said below
- tile_source: int32 [64, 4, 256], P('dom', 'rep'), may hold values from 0 to 95, as said below
- tile_weights: bfloat16 [64, 4, 256, 128, 128], P('dom', 'rep'), may hold values from -0.125 to 0.125
Outputs:
- activated: bfloat16 [524288, 256], P(('dom', 'rep'))
- feature_grad: bfloat16 [524288, 128], P(('dom', 'rep'))
- weight_grad: float32 [128, 256], replicated
The draws below stay inside these ranges and needn't reach their ends.
Inputs may be any that keep to these rules, and one draw needn't show every extreme that they name: Within one list send_rows[o, d] the rows are distinct and increasing; entries at slots c >= send_count[o, d] are ignored. send_count[o, o] is 0. Every owner sends exactly 64 rows to some partition, and every partition receives exactly 64 rows from some owner. `tile_target`: pairs of target and source tiles may repeat. `tile_source`: every halo source tile (64 to 95) is named by some tile of every group.
All inputs are finite; a program needn't handle non-finite values.
Results may differ from the reference program's by a relative error of at most 0.006.
Values may be sent and summed in bfloat16 or wider, within the bound.
A program may use at most 128 MiB of HBM per device.

```python
import jax
import jax.numpy as jnp
from jax import lax

FEAT = 128
HIDDEN_SIZE = 256
TILE = 128
TILES_PER = 16
CAP = 64
TGT_DEV = 2048
NODES_DEV = 8192
NODES = 524288
TGT_TILES = 16
LOCAL_TILES = 64
HALO_TILES = 32
SRC_TILES = 96
NTILE = 256
N_DOM = 64
N_REP = 4


def draw_send_count(key, part):
    first, second, third = jax.random.split(jax.random.fold_in(key, 11), 3)
    one = jax.random.randint(first, (N_DOM, N_DOM), 0, CAP + 1)
    two = jax.random.randint(second, (N_DOM, N_DOM), 0, CAP + 1)
    counts = jnp.maximum(one, two)
    offset = jax.random.randint(third, (), 1, N_DOM)
    owners = jnp.arange(N_DOM)[:, None]
    dests = jnp.arange(N_DOM)[None, :]
    counts = jnp.where((owners + offset) % N_DOM == dests, CAP, counts)
    counts = jnp.where(owners == dests, 0, counts)
    return counts.astype(jnp.int32)


def draw_send_rows(key, part):
    first, second = jax.random.split(jax.random.fold_in(key, 23), 2)
    stride = jax.random.randint(first, (N_DOM, N_DOM, 1), 1, NODES_DEV // CAP)
    base = jax.random.randint(second, (N_DOM, N_DOM, 1), 0, NODES_DEV - (CAP - 1) * stride)
    rows = base + jnp.arange(CAP)[None, None, :] * stride
    return rows.astype(jnp.int32)


def draw_tile_target(key, part):
    picked = jax.random.randint(jax.random.fold_in(key, 37), (N_DOM, N_REP, NTILE), 0, TGT_TILES)
    return picked.astype(jnp.int32)


def draw_tile_source(key, part):
    picked = jax.random.randint(jax.random.fold_in(key, 41), (N_DOM, N_REP, NTILE), 0, SRC_TILES)
    place = jnp.arange(NTILE)[None, None, :]
    picked = jnp.where(place < HALO_TILES, LOCAL_TILES + place, picked)
    return picked.astype(jnp.int32)


def block_levels(key, extent, cuts, low, largest):
    level = 1.0
    for dim, blocks in cuts:
        heights = jax.random.uniform(jax.random.fold_in(jax.random.fold_in(key, 6), dim), (blocks,), jnp.float32, low / len(cuts), largest / len(cuts))
        level = level * jnp.repeat(jnp.exp(heights), extent[dim] // blocks).reshape((-1,) + (1,) * (len(extent) - 1 - dim))
    return level


def noise(stream_key, shape, deviation, bound, pieces=(), held_as=jnp.bfloat16):
    loudness = block_levels(stream_key, shape, pieces, -0.22, 0.18) if pieces else 1.0
    entries = jax.random.normal(stream_key, shape, jnp.float32) * deviation * loudness
    return jnp.minimum(jnp.maximum(entries, -bound), bound).astype(held_as)


def setup_inputs(seed: int = 0) -> dict:
    key_list = jax.random.split(jax.random.key(seed), 9)
    features = noise(key_list[0], (NODES, FEAT), 1.0, 6.0, ((0, 64),))
    weight = noise(key_list[1], (FEAT, HIDDEN_SIZE), FEAT ** -0.5, 0.5)
    out_grad = noise(key_list[2], (NODES, HIDDEN_SIZE), 1.0, 6.0, ((0, 256),))
    send_rows = draw_send_rows(jax.random.fold_in(key_list[8], 71), 0)
    send_count = draw_send_count(jax.random.fold_in(key_list[8], 71), 0)
    tile_target = draw_tile_target(jax.random.fold_in(key_list[8], 71), 0)
    tile_source = draw_tile_source(jax.random.fold_in(key_list[8], 71), 0)
    tile_weights = noise(key_list[7], (N_DOM, N_REP, NTILE, TILE, TILE), (TILES_PER * TILE) ** -0.5, 0.125, ((0, 64), (1, 4)))
    return dict(features=features, weight=weight, out_grad=out_grad, send_rows=send_rows, send_count=send_count, tile_target=tile_target, tile_source=tile_source, tile_weights=tile_weights)


def device_pass(sources, weights_tiles, targets, anchors, grad_rows, weight):
    tile = weights_tiles.shape[-1]
    feat = sources.shape[1]
    blocks = sources.reshape(-1, tile, feat)[anchors]
    prods = jnp.einsum("tij,tjf->tif", weights_tiles.astype(jnp.float32), blocks.astype(jnp.float32), precision=lax.Precision.HIGHEST)
    gathered = jax.ops.segment_sum(prods, targets, num_segments=TGT_TILES).reshape(TGT_DEV, feat).astype(jnp.bfloat16)
    pre = jnp.dot(gathered, weight, preferred_element_type=jnp.float32)
    activated = jax.nn.silu(pre).astype(jnp.bfloat16)
    sigma = jax.nn.sigmoid(pre)
    slope = sigma * (1.0 + pre * (1.0 - sigma))
    pre_grad = (grad_rows.astype(jnp.float32) * slope).astype(jnp.bfloat16)
    weight_part = jnp.dot(gathered.T, pre_grad, preferred_element_type=jnp.float32)
    agg_grad = jnp.dot(pre_grad, weight.T, preferred_element_type=jnp.float32).astype(jnp.bfloat16)
    dblocks = agg_grad.reshape(TGT_TILES, tile, feat)[targets]
    backward = jnp.einsum("tij,tif->tjf", weights_tiles.astype(jnp.float32), dblocks.astype(jnp.float32), precision=lax.Precision.HIGHEST)
    source_grad = jax.ops.segment_sum(backward, anchors, num_segments=SRC_TILES).reshape(-1, feat)
    return activated, weight_part, source_grad


def reference(features, weight, out_grad, send_rows, send_count, tile_target, tile_source, tile_weights):
    owned = features.reshape(N_DOM, NODES_DEV, FEAT)
    slots = jnp.arange(CAP, dtype=jnp.int32)
    valid = slots[None, None, :] < send_count[:, :, None]
    sent = jax.vmap(lambda block, index: block[index])(owned, send_rows)
    sent = jnp.where(valid[..., None], sent, jnp.zeros((), jnp.bfloat16))
    halo = jnp.transpose(sent, (1, 0, 2, 3)).reshape(N_DOM, N_DOM * CAP, FEAT)
    grads = out_grad.reshape(N_DOM, N_REP, TGT_DEV, HIDDEN_SIZE)

    def one_part(carry, part):
        sources = jnp.concatenate([owned[part], halo[part]], axis=0)
        outputs = []
        total = jnp.zeros((SRC_TILES * TILE, FEAT), jnp.float32)
        for rank in range(N_REP):
            act, part_w, part_s = device_pass(sources, tile_weights[part, rank], tile_target[part, rank], tile_source[part, rank], grads[part, rank], weight)
            outputs.append(act)
            carry = carry + part_w
            total = total + part_s
        return carry, (jnp.stack(outputs), total)

    weight_grad, (acts, totals) = lax.scan(one_part, jnp.zeros((FEAT, HIDDEN_SIZE), jnp.float32), jnp.arange(N_DOM, dtype=jnp.int32))
    local = totals[:, :NODES_DEV]
    returned = totals[:, NODES_DEV:].reshape(N_DOM, N_DOM, CAP, FEAT)
    returned = jnp.transpose(returned, (1, 0, 2, 3))
    returned = jnp.where(valid[..., None], returned, jnp.zeros((), jnp.float32))
    local = jax.vmap(lambda acc, index, rows: acc.at[index.reshape(-1)].add(rows.reshape(-1, FEAT)))(local, send_rows, returned)
    return acts.reshape(NODES, HIDDEN_SIZE), local.reshape(NODES, FEAT).astype(jnp.bfloat16), weight_grad
```

```python
import functools

import jax
import jax.numpy as jnp
from jax import lax
from jax.experimental import pallas as pl
from jax.experimental.pallas import tpu as pltpu
from jax.sharding import PartitionSpec as P

F32 = jnp.float32
BF16 = jnp.bfloat16
TILE = 128
FEAT = 128
HID = 256
CAP = 64
NDOM = 64
NREP = 4
Q = CAP // NREP
ROWS = 8192
TGT = 16
NT = 256
SRC = 96
LOCAL = 64
CHUNKS = 16
PER = NT // CHUNKS

VMEM = pl.BlockSpec(memory_space=pltpu.VMEM)
SMEM = pl.BlockSpec(memory_space=pltpu.SMEM)
ANY = pl.BlockSpec(memory_space=pl.ANY)
MESH = pl.DeviceIdType.MESH


def peer_id(d, r):
    return (d, r)


def gather_kernel(rows, counts, feats, out, wide, picked):
    rep = lax.axis_index("rep")
    wide[pl.ds(0, ROWS), :] = feats[...].astype(F32)
    wide[pl.ds(ROWS, 8), :] = jnp.zeros((8, FEAT), F32)

    @pl.loop(0, NDOM)
    def _(d):
        live = counts[0, d]
        for c in range(Q):
            slot = rep * Q + c
            row = jnp.where(slot < live, rows[0, d, slot], ROWS)
            picked[pl.ds(d * Q + c, 1), :] = wide[pl.ds(row, 1), :]

    out[...] = picked[...].reshape(NDOM, Q, FEAT).astype(BF16)


def gather_rows(rows, counts, feats):
    return pl.pallas_call(
        gather_kernel,
        out_shape=jax.ShapeDtypeStruct((NDOM, Q, FEAT), BF16),
        in_specs=[SMEM, SMEM, VMEM],
        out_specs=VMEM,
        scratch_shapes=[
            pltpu.VMEM((ROWS + 8, FEAT), F32),
            pltpu.VMEM((NDOM * Q, FEAT), F32),
        ],
        name="gather_rows",
    )(rows, counts, feats)


def greet_all(me_d, me_r):
    barrier = pltpu.get_barrier_semaphore()

    @pl.loop(1, NDOM)
    def _(k):
        pl.semaphore_signal(
            barrier, inc=1, device_id=peer_id(lax.rem(me_d + k, NDOM), me_r), device_id_type=MESH
        )

    for k in range(1, NREP):
        pl.semaphore_signal(
            barrier, inc=1, device_id=peer_id(me_d, lax.rem(me_r + k, NREP)), device_id_type=MESH
        )
    pl.semaphore_wait(barrier, NDOM - 1 + NREP - 1)


def halo_kernel(send, halo, own_sem, send_sem, recv_sem, share_send, share_recv):
    me_d = lax.axis_index("dom")
    me_r = lax.axis_index("rep")
    greet_all(me_d, me_r)

    def to(k):
        d = lax.rem(me_d + k, NDOM)
        return pltpu.make_async_remote_copy(
            src_ref=send.at[d],
            dst_ref=halo.at[me_d, me_r],
            send_sem=send_sem.at[k],
            recv_sem=recv_sem.at[k],
            device_id=peer_id(d, me_r),
            device_id_type=MESH,
        )

    def came(k):
        d = lax.rem(me_d + NDOM - k, NDOM)
        return pltpu.make_async_remote_copy(
            src_ref=send.at[d],
            dst_ref=halo.at[d, me_r],
            send_sem=send_sem.at[k],
            recv_sem=recv_sem.at[k],
            device_id=peer_id(d, me_r),
            device_id_type=MESH,
        )

    own = pltpu.make_async_copy(send.at[me_d], halo.at[me_d, me_r], own_sem)
    own.start()

    @pl.loop(1, NDOM)
    def _(k):
        to(k).start()

    own.wait()

    @pl.loop(1, NDOM)
    def _(k):
        came(k).wait_recv()

    shares = []
    for k in range(1, NREP):
        share = pltpu.make_async_remote_copy(
            src_ref=halo.at[:, me_r],
            dst_ref=halo.at[:, me_r],
            send_sem=share_send.at[k],
            recv_sem=share_recv.at[k],
            device_id=peer_id(me_d, lax.rem(me_r + k, NREP)),
            device_id_type=MESH,
        )
        share.start()
        shares.append(share)

    @pl.loop(1, NDOM)
    def _(k):
        to(k).wait_send()

    for k in range(1, NREP):
        r = lax.rem(me_r + NREP - k, NREP)
        pltpu.make_async_remote_copy(
            src_ref=halo.at[:, r],
            dst_ref=halo.at[:, r],
            send_sem=share_send.at[k],
            recv_sem=share_recv.at[k],
            device_id=peer_id(me_d, r),
            device_id_type=MESH,
        ).wait_recv()
    for share in shares:
        share.wait_send()


def exchange_halo(send):
    return pl.pallas_call(
        halo_kernel,
        out_shape=jax.ShapeDtypeStruct((NDOM, NREP, Q, FEAT), BF16),
        in_specs=[VMEM],
        out_specs=VMEM,
        scratch_shapes=[
            pltpu.SemaphoreType.DMA,
            pltpu.SemaphoreType.DMA((NDOM,)),
            pltpu.SemaphoreType.DMA((NDOM,)),
            pltpu.SemaphoreType.DMA((NREP,)),
            pltpu.SemaphoreType.DMA((NREP,)),
        ],
        compiler_params=pltpu.CompilerParams(collective_id=0, has_side_effects=True),
        name="exchange_halo",
    )(send)


def layer_kernel(
    targets, anchors, feats, halo, tiles, grads, weight,
    act_out, local_out, halo_out, wgrad_out,
    src, wt, og, agg, gt, sg, act, sgb, wg,
    src_sem, wt_sem, og_sem, out_sem,
):
    loads = [
        pltpu.make_async_copy(feats, src.at[pl.ds(0, LOCAL)], src_sem.at[0]),
        pltpu.make_async_copy(halo, src.at[pl.ds(LOCAL, SRC - LOCAL)], src_sem.at[1]),
    ]
    for load in loads:
        load.start()

    def tile_load(c):
        part = pl.ds(c * PER, PER)
        return pltpu.make_async_copy(tiles.at[part], wt.at[part], wt_sem.at[c])

    for c in range(CHUNKS):
        tile_load(c).start()
    grad_load = pltpu.make_async_copy(grads, og, og_sem)
    grad_load.start()

    agg[...] = jnp.zeros_like(agg)
    sg[...] = jnp.zeros_like(sg)
    wg[...] = jnp.zeros_like(wg)
    for load in loads:
        load.wait()

    @pl.loop(0, CHUNKS)
    def _(c):
        tile_load(c).wait()
        for u in range(PER):
            t = c * PER + u
            prod = jnp.dot(wt[t], src[anchors[0, 0, t]], preferred_element_type=F32)
            k = targets[0, 0, t]
            agg[k] = agg[k] + prod

    grad_load.wait()

    @pl.loop(0, TGT)
    def _(k):
        gathered = agg[k].astype(BF16)
        pre = jnp.dot(gathered, weight[...], preferred_element_type=F32)
        sigma = jax.nn.sigmoid(pre)
        part = pl.ds(pl.multiple_of(k * TILE, TILE), TILE)
        act[part, :] = (pre * sigma).astype(BF16)
        slope = sigma * (1.0 + pre * (1.0 - sigma))
        pre_grad = (og[part, :].astype(F32) * slope).astype(BF16)
        wg[...] += lax.dot_general(
            gathered, pre_grad, (((0,), (0,)), ((), ())), preferred_element_type=F32
        )
        gt[k] = lax.dot_general(
            weight[...], pre_grad, (((1,), (1,)), ((), ())), preferred_element_type=F32
        ).astype(BF16)

    act_save = pltpu.make_async_copy(act, act_out, out_sem.at[0])
    act_save.start()
    wgrad_out[...] = jnp.concatenate([wg[:, :TILE], wg[:, TILE:]], axis=0)

    @pl.loop(0, CHUNKS)
    def _(c):
        for u in range(PER):
            t = c * PER + u
            prod = jnp.dot(gt[targets[0, 0, t]], wt[t], preferred_element_type=F32)
            s = anchors[0, 0, t]
            sg[s] = sg[s] + prod

    one = (
        lax.broadcasted_iota(jnp.int32, (TILE, TILE), 0)
        == lax.broadcasted_iota(jnp.int32, (TILE, TILE), 1)
    ).astype(F32).astype(BF16)

    @pl.loop(0, SRC // 8)
    def _(c):
        for u in range(8):
            s = c * 8 + u
            sgb[s] = lax.dot_general(
                one, sg[s].astype(BF16), (((1,), (1,)), ((), ())), preferred_element_type=F32
            ).astype(BF16)

    saves = [
        pltpu.make_async_copy(sgb.at[pl.ds(0, LOCAL)], local_out, out_sem.at[1]),
        pltpu.make_async_copy(sgb.at[pl.ds(LOCAL, SRC - LOCAL)], halo_out, out_sem.at[2]),
    ]
    for save in saves:
        save.start()
    act_save.wait()
    for save in saves:
        save.wait()


def layer(targets, anchors, feats, halo, tiles, grads, weight):
    return pl.pallas_call(
        layer_kernel,
        out_shape=(
            jax.ShapeDtypeStruct((TGT * TILE, HID), BF16),
            jax.ShapeDtypeStruct((LOCAL, TILE, FEAT), BF16),
            jax.ShapeDtypeStruct((SRC - LOCAL, TILE, FEAT), BF16),
            jax.ShapeDtypeStruct((2 * FEAT, TILE), F32),
        ),
        in_specs=[SMEM, SMEM, ANY, ANY, ANY, ANY, VMEM],
        out_specs=(ANY, ANY, ANY, VMEM),
        scratch_shapes=[
            pltpu.VMEM((SRC, TILE, FEAT), BF16),
            pltpu.VMEM((NT, TILE, TILE), BF16),
            pltpu.VMEM((TGT * TILE, HID), BF16),
            pltpu.VMEM((TGT, TILE, FEAT), F32),
            pltpu.VMEM((TGT, FEAT, TILE), BF16),
            pltpu.VMEM((SRC, FEAT, TILE), F32),
            pltpu.VMEM((TGT * TILE, HID), BF16),
            pltpu.VMEM((SRC, TILE, FEAT), BF16),
            pltpu.VMEM((FEAT, HID), F32),
            pltpu.SemaphoreType.DMA((2,)),
            pltpu.SemaphoreType.DMA((CHUNKS,)),
            pltpu.SemaphoreType.DMA,
            pltpu.SemaphoreType.DMA((3,)),
        ],
        name="layer",
    )(targets, anchors, feats, halo, tiles, grads, weight)


def return_kernel(
    part, wpart, back, wrow,
    inbox, sums, winbox, wsums,
    own_sem, rs_send, rs_recv, send_sem, recv_sem,
):
    me_d = lax.axis_index("dom")
    me_r = lax.axis_index("rep")
    greet_all(me_d, me_r)

    def reduce_to(k):
        r = lax.rem(me_r + k, NREP)
        dev = peer_id(me_d, r)
        return (
            pltpu.make_async_remote_copy(
                src_ref=part.at[:, r], dst_ref=inbox.at[k], send_sem=rs_send.at[0, k],
                recv_sem=rs_recv.at[0, k], device_id=dev, device_id_type=MESH,
            ),
            pltpu.make_async_remote_copy(
                src_ref=wpart.at[r], dst_ref=winbox.at[k], send_sem=rs_send.at[1, k],
                recv_sem=rs_recv.at[1, k], device_id=dev, device_id_type=MESH,
            ),
        )

    for k in range(1, NREP):
        for copy in reduce_to(k):
            copy.start()
    own_halo = pltpu.make_async_copy(part.at[:, me_r], inbox.at[0], own_sem.at[0])
    own_halo.start()
    own_w = pltpu.make_async_copy(wpart.at[me_r], winbox.at[0], own_sem.at[1])
    own_w.start()
    own_halo.wait()
    own_w.wait()
    for k in range(1, NREP):
        for copy in reduce_to(k):
            copy.wait_recv()

    wsums[...] = (winbox[0] + winbox[1] + winbox[2] + winbox[3]).reshape(NDOM, 1, TILE)
    sums[...] = (
        inbox[0].astype(F32) + inbox[1].astype(F32) + inbox[2].astype(F32) + inbox[3].astype(F32)
    ).astype(BF16)

    def to(k):
        d = lax.rem(me_d + k, NDOM)
        dev = peer_id(d, me_r)
        return (
            pltpu.make_async_remote_copy(
                src_ref=sums.at[d], dst_ref=back.at[me_d], send_sem=send_sem.at[0, k],
                recv_sem=recv_sem.at[0, k], device_id=dev, device_id_type=MESH,
            ),
            pltpu.make_async_remote_copy(
                src_ref=wsums.at[d], dst_ref=wrow.at[me_d], send_sem=send_sem.at[1, k],
                recv_sem=recv_sem.at[1, k], device_id=dev, device_id_type=MESH,
            ),
        )

    def came(k):
        d = lax.rem(me_d + NDOM - k, NDOM)
        dev = peer_id(d, me_r)
        return (
            pltpu.make_async_remote_copy(
                src_ref=sums.at[d], dst_ref=back.at[d], send_sem=send_sem.at[0, k],
                recv_sem=recv_sem.at[0, k], device_id=dev, device_id_type=MESH,
            ),
            pltpu.make_async_remote_copy(
                src_ref=wsums.at[d], dst_ref=wrow.at[d], send_sem=send_sem.at[1, k],
                recv_sem=recv_sem.at[1, k], device_id=dev, device_id_type=MESH,
            ),
        )

    @pl.loop(1, NDOM)
    def _(k):
        for copy in to(k):
            copy.start()

    own_back = pltpu.make_async_copy(sums.at[me_d], back.at[me_d], own_sem.at[0])
    own_back.start()
    own_row = pltpu.make_async_copy(wsums.at[me_d], wrow.at[me_d], own_sem.at[1])
    own_row.start()
    own_back.wait()
    own_row.wait()

    @pl.loop(1, NDOM)
    def _(k):
        for copy in came(k):
            copy.wait_recv()
        for copy in to(k):
            copy.wait_send()

    for k in range(1, NREP):
        for copy in reduce_to(k):
            copy.wait_send()


def return_halo(part, wpart):
    return pl.pallas_call(
        return_kernel,
        out_shape=(
            jax.ShapeDtypeStruct((NDOM, Q, FEAT), BF16),
            jax.ShapeDtypeStruct((NDOM, 1, TILE), F32),
        ),
        in_specs=[VMEM, VMEM],
        out_specs=(VMEM, VMEM),
        scratch_shapes=[
            pltpu.VMEM((NREP, NDOM, Q, FEAT), BF16),
            pltpu.VMEM((NDOM, Q, FEAT), BF16),
            pltpu.VMEM((NREP, NDOM, TILE), F32),
            pltpu.VMEM((NDOM, 1, TILE), F32),
            pltpu.SemaphoreType.DMA((2,)),
            pltpu.SemaphoreType.DMA((2, NREP)),
            pltpu.SemaphoreType.DMA((2, NREP)),
            pltpu.SemaphoreType.DMA((2, NDOM)),
            pltpu.SemaphoreType.DMA((2, NDOM)),
        ],
        compiler_params=pltpu.CompilerParams(collective_id=1, has_side_effects=True),
        name="return_halo",
    )(part, wpart)


def scatter_kernel(rows, counts, local, back, wrow, out, wrow_out, wide, news):
    rep = lax.axis_index("rep")
    wide[pl.ds(0, ROWS), :] = local[...].astype(F32)
    wide[pl.ds(ROWS, Q), :] = jnp.zeros((Q, FEAT), F32)
    news[...] = back[...].reshape(NDOM * Q, FEAT).astype(F32)
    wrow_out[...] = jnp.sum(wrow[...], axis=0)

    @pl.loop(0, NDOM)
    def _(d):
        live = counts[0, d]
        places = []
        for c in range(Q):
            slot = rep * Q + c
            places.append(jnp.where(slot < live, rows[0, d, slot], ROWS + c))
        olds = [wide[pl.ds(row, 1), :] for row in places]
        for c, row in enumerate(places):
            wide[pl.ds(row, 1), :] = olds[c] + news[pl.ds(d * Q + c, 1), :]

    out[...] = wide[pl.ds(0, ROWS), :].astype(BF16)


def scatter_rows(rows, counts, local, back, wrow):
    return pl.pallas_call(
        scatter_kernel,
        out_shape=(
            jax.ShapeDtypeStruct((ROWS, FEAT), BF16),
            jax.ShapeDtypeStruct((1, TILE), F32),
        ),
        in_specs=[SMEM, SMEM, VMEM, VMEM, VMEM],
        out_specs=(VMEM, VMEM),
        scratch_shapes=[
            pltpu.VMEM((ROWS + Q, FEAT), F32),
            pltpu.VMEM((NDOM * Q, FEAT), F32),
        ],
        name="scatter_rows",
    )(rows, counts, local, back, wrow)


def final_kernel(
    part, wrow, out, wout, inbox,
    own_sem, rs_send, rs_recv, send_sem, recv_sem, ag_send, ag_recv,
):
    me_d = lax.axis_index("dom")
    me_r = lax.axis_index("rep")
    greet_all(me_d, me_r)

    def reduce_to(k):
        r = lax.rem(me_r + k, NREP)
        return pltpu.make_async_remote_copy(
            src_ref=part.at[r], dst_ref=inbox.at[k], send_sem=rs_send.at[k],
            recv_sem=rs_recv.at[k], device_id=peer_id(me_d, r), device_id_type=MESH,
        )

    def row_to(k):
        d = lax.rem(me_d + k, NDOM)
        return pltpu.make_async_remote_copy(
            src_ref=wrow, dst_ref=wout.at[me_r, me_d], send_sem=send_sem.at[k],
            recv_sem=recv_sem.at[k], device_id=peer_id(d, me_r), device_id_type=MESH,
        )

    def row_came(k):
        d = lax.rem(me_d + NDOM - k, NDOM)
        return pltpu.make_async_remote_copy(
            src_ref=wrow, dst_ref=wout.at[me_r, d], send_sem=send_sem.at[k],
            recv_sem=recv_sem.at[k], device_id=peer_id(d, me_r), device_id_type=MESH,
        )

    def spread(k, r):
        return pltpu.make_async_remote_copy(
            src_ref=wout.at[me_r], dst_ref=wout.at[r], send_sem=ag_send.at[k],
            recv_sem=ag_recv.at[k], device_id=peer_id(me_d, lax.rem(me_r + k, NREP)),
            device_id_type=MESH,
        )

    @pl.loop(1, NDOM)
    def _(k):
        row_to(k).start()

    for k in range(1, NREP):
        reduce_to(k).start()
    own = pltpu.make_async_copy(wrow, wout.at[me_r, me_d], own_sem)
    own.start()
    own.wait()

    @pl.loop(1, NDOM)
    def _(k):
        row_came(k).wait_recv()

    for k in range(1, NREP):
        spread(k, me_r).start()

    @pl.loop(1, NDOM)
    def _(k):
        row_to(k).wait_send()

    for k in range(1, NREP):
        reduce_to(k).wait_recv()
    out[...] = (
        part[me_r].astype(F32) + inbox[1].astype(F32) + inbox[2].astype(F32) + inbox[3].astype(F32)
    ).astype(BF16)
    for k in range(1, NREP):
        reduce_to(k).wait_send()
        spread(k, lax.rem(me_r + NREP - k, NREP)).wait_recv()
        spread(k, me_r).wait_send()


def final_sums(part, wrow):
    rows = ROWS // NREP
    return pl.pallas_call(
        final_kernel,
        out_shape=(
            jax.ShapeDtypeStruct((rows, FEAT), BF16),
            jax.ShapeDtypeStruct((NREP, NDOM, 1, TILE), F32),
        ),
        in_specs=[VMEM, VMEM],
        out_specs=(VMEM, VMEM),
        scratch_shapes=[
            pltpu.VMEM((NREP, rows, FEAT), BF16),
            pltpu.SemaphoreType.DMA,
            pltpu.SemaphoreType.DMA((NREP,)),
            pltpu.SemaphoreType.DMA((NREP,)),
            pltpu.SemaphoreType.DMA((NDOM,)),
            pltpu.SemaphoreType.DMA((NDOM,)),
            pltpu.SemaphoreType.DMA((NREP,)),
            pltpu.SemaphoreType.DMA((NREP,)),
        ],
        compiler_params=pltpu.CompilerParams(collective_id=2, has_side_effects=True),
        name="final_sums",
    )(part, wrow)


def shards(
    features, weight, out_grad, send_rows, send_count, tile_target, tile_source, tile_weights
):
    send = gather_rows(send_rows, send_count, features)
    halo = exchange_halo(send)
    activated, local, halo_grad, wpart = layer(
        tile_target,
        tile_source,
        features.reshape(LOCAL, TILE, FEAT),
        halo.reshape(SRC - LOCAL, TILE, FEAT),
        tile_weights.reshape(NT, TILE, TILE),
        out_grad,
        weight,
    )
    back, wrows = return_halo(
        halo_grad.reshape(NDOM, NREP, Q, FEAT), wpart.reshape(NREP, NDOM, TILE)
    )
    node_part, wrow = scatter_rows(
        send_rows, send_count, local.reshape(ROWS, FEAT), back, wrows
    )
    node_grad, wall = final_sums(node_part.reshape(NREP, ROWS // NREP, FEAT), wrow)
    wall = wall.reshape(2, FEAT, TILE)
    weight_grad = jnp.concatenate([wall[0], wall[1]], axis=1)
    return (activated, node_grad, weight_grad)


def solution(mesh):
    both = ("dom", "rep")
    in_specs = (
        P("dom", None),
        P(),
        P(both, None),
        P("dom", None, None),
        P("dom", None),
        P("dom", "rep", None),
        P("dom", "rep", None),
        P("dom", "rep", None, None, None),
    )
    out_specs = (P(both, None), P(both, None), P())
    return jax.shard_map(
        shards, mesh=mesh, in_specs=in_specs, out_specs=out_specs, check_vma=False
    )
```

```python
import functools

import jax
import jax.numpy as jnp
from jax import lax
from jax.experimental import pallas as pl
from jax.experimental.pallas import tpu as pltpu
from jax.sharding import PartitionSpec as P

F32 = jnp.float32
BF16 = jnp.bfloat16
TILE = 128
FEAT = 128
HID = 256
CAP = 64
NDOM = 64
NREP = 4
Q = CAP // NREP
ROWS = 8192
TGT = 16
NT = 256
SRC = 96
LOCAL = 64
CHUNKS = 16
PER = NT // CHUNKS

VMEM = pl.BlockSpec(memory_space=pltpu.VMEM)
SMEM = pl.BlockSpec(memory_space=pltpu.SMEM)
ANY = pl.BlockSpec(memory_space=pl.ANY)
MESH = pl.DeviceIdType.MESH


NZ = 8
PLANE = NDOM // NZ
HALF = PLANE // 2
PARTS = 4
DENSE = 4
SAVES = 3
LISTS = 4
PIECES = 4
WROWS = 2 * FEAT // NDOM


def place():
    me_d = lax.axis_index("dom")
    me_r = lax.axis_index("rep")
    right = lax.rem(me_r + 1, NREP)
    across = lax.rem(me_r + 2, NREP)
    left = lax.rem(me_r + 3, NREP)
    return me_d, me_r, right, across, left


def remote(src, dst, send_sem, recv_sem, dev):
    return pltpu.make_async_remote_copy(
        src_ref=src, dst_ref=dst, send_sem=send_sem, recv_sem=recv_sem,
        device_id=dev, device_id_type=MESH,
    )


def greet(devices):
    barrier = pltpu.get_barrier_semaphore()
    for dev in devices:
        pl.semaphore_signal(barrier, inc=1, device_id=dev, device_id_type=MESH)


def greet_dom(me_d, me_r):
    barrier = pltpu.get_barrier_semaphore()

    @pl.loop(1, NDOM)
    def _(k):
        pl.semaphore_signal(
            barrier, inc=1, device_id=(lax.rem(me_d + k, NDOM), me_r), device_id_type=MESH
        )


def greeted(count):
    pl.semaphore_wait(pltpu.get_barrier_semaphore(), count)


def plane_step(i):
    odd = lax.rem(i, 2)
    return lax.rem(4 + odd * ((i + 1) // 2) - (1 - odd) * (i // 2), NZ)


def near_step(i):
    return plane_step(NZ - 1 - i)


def ahead(me_d, step, place):
    z = lax.rem(me_d // PLANE + step, NZ)
    return z * PLANE + lax.rem(lax.rem(me_d, PLANE) + place, PLANE)


def behind(me_d, step, place):
    z = lax.rem(me_d // PLANE + NZ - step, NZ)
    return z * PLANE + lax.rem(lax.rem(me_d, PLANE) + PLANE - place, PLANE)


def plane_rows(me_d, step):
    return pl.ds(lax.rem(me_d // PLANE + step, NZ) * PLANE, PLANE)


OWN = NDOM - PLANE


def others(body):
    @pl.loop(0, OWN)
    def _(n):
        body(n)

    @pl.loop(OWN + 1, NDOM)
    def _(n):
        body(n)


def halo_kernel(
    rows, counts, feats, halo,
    raw, wide, picked, send,
    load_sem, own_sem, send_sem, recv_sem, ring_send, ring_recv,
):
    me_d, me_r, right, across, left = place()
    greet_dom(me_d, me_r)
    greet([(me_d, right), (me_d, left), (me_d, across)])

    load = pltpu.make_async_copy(feats, raw, load_sem)
    load.start()
    load.wait()
    wide[pl.ds(0, ROWS), :] = raw[...].astype(F32)
    wide[pl.ds(ROWS, 8), :] = jnp.zeros((8, FEAT), F32)

    @pl.loop(0, NDOM // LISTS)
    def _(g):
        for u in range(LISTS):
            d = g * LISTS + u
            live = counts[0, d]
            for c in range(Q):
                slot = me_r * Q + c
                row = jnp.where(slot < live, rows[0, d, slot], ROWS)
                picked[pl.ds(d * Q + c, 1), :] = wide[pl.ds(row, 1), :]

    send[...] = picked[...].reshape(NDOM, Q, FEAT).astype(BF16)
    greeted(NDOM - 1 + 3)

    def to(n):
        d = behind(me_d, near_step(n // PLANE), lax.rem(n, PLANE))
        return remote(
            send.at[d], halo.at[me_r, me_d], send_sem.at[n], recv_sem.at[n], (d, me_r)
        )

    def came(n):
        d = ahead(me_d, near_step(n // PLANE), lax.rem(n, PLANE))
        return remote(send.at[d], halo.at[me_r, d], send_sem.at[n], recv_sem.at[n], (d, me_r))

    own = pltpu.make_async_copy(send.at[me_d], halo.at[me_r, me_d], own_sem)
    own.start()

    @pl.loop(1, NDOM)
    def _(n):
        to(n).start()

    def share(i, k, owner):
        block = halo.at[owner, plane_rows(me_d, near_step(i))]
        dev = (me_d, lax.rem(me_r + k, NREP))
        return remote(block, block, ring_send.at[i, k], ring_recv.at[i, k], dev)

    own.wait()

    @pl.loop(0, NZ)
    def _(i):
        @pl.loop(jnp.maximum(i * PLANE, 1), (i + 1) * PLANE)
        def _(n):
            came(n).wait_recv()

        for k in (2, 1, 3):
            share(i, k, me_r).start()

    @pl.loop(1, NDOM)
    def _(n):
        to(n).wait_send()

    @pl.loop(0, NZ)
    def _(i):
        for k in range(1, NREP):
            share(i, k, lax.rem(me_r + NREP - k, NREP)).wait_recv()
            share(i, k, me_r).wait_send()


def exchange_halo(rows, counts, feats):
    return pl.pallas_call(
        halo_kernel,
        out_shape=jax.ShapeDtypeStruct((NREP, NDOM, Q, FEAT), BF16),
        in_specs=[SMEM, SMEM, ANY],
        out_specs=VMEM,
        scratch_shapes=[
            pltpu.VMEM((ROWS, FEAT), BF16),
            pltpu.VMEM((ROWS + 8, FEAT), F32),
            pltpu.VMEM((NDOM * Q, FEAT), F32),
            pltpu.VMEM((NDOM, Q, FEAT), BF16),
            pltpu.SemaphoreType.DMA,
            pltpu.SemaphoreType.DMA,
            pltpu.SemaphoreType.DMA((NDOM,)),
            pltpu.SemaphoreType.DMA((NDOM,)),
            pltpu.SemaphoreType.DMA((NZ, NREP)),
            pltpu.SemaphoreType.DMA((NZ, NREP)),
        ],
        compiler_params=pltpu.CompilerParams(collective_id=0, has_side_effects=True),
        name="exchange_halo",
    )(rows, counts, feats)


def layer_kernel(
    targets, anchors, feats, halo, tiles, grads, weight,
    act_out, sgt_out, wgrad_out,
    src, wt, og, agg, gt, sg, act, sgb, wg,
    src_sem, wt_sem, og_sem, out_sem,
):
    loads = [
        pltpu.make_async_copy(feats, src.at[pl.ds(0, 2 * LOCAL)], src_sem.at[NREP])
    ] + [
        pltpu.make_async_copy(halo.at[r], src.at[pl.ds(2 * LOCAL, NDOM), r], src_sem.at[r])
        for r in range(NREP)
    ]
    for load in loads:
        load.start()

    def tile_load(c):
        part = pl.ds(c * PER, PER)
        return pltpu.make_async_copy(tiles.at[part], wt.at[part], wt_sem.at[c])

    for c in range(CHUNKS):
        tile_load(c).start()
    grad_load = pltpu.make_async_copy(grads, og, og_sem)
    grad_load.start()

    agg[...] = jnp.zeros_like(agg)
    sg[...] = jnp.zeros_like(sg)
    wg[...] = jnp.zeros_like(wg)
    for load in loads:
        load.wait()

    @pl.loop(0, CHUNKS)
    def _(c):
        tile_load(c).wait()
        for u in range(PER):
            t = c * PER + u
            block = src[pl.ds(anchors[0, 0, t] * 2, 2)].reshape(TILE, FEAT)
            prod = jnp.dot(wt[t], block, preferred_element_type=F32)
            k = targets[0, 0, t]
            agg[k] = agg[k] + prod

    grad_load.wait()

    @pl.loop(0, TGT // DENSE)
    def _(c):
        total = wg[...]
        for u in range(DENSE):
            k = c * DENSE + u
            gathered = agg[k].astype(BF16)
            pre = jnp.dot(gathered, weight[...], preferred_element_type=F32)
            sigma = jax.nn.sigmoid(pre)
            part = pl.ds(pl.multiple_of(k * TILE, TILE), TILE)
            act[part, :] = (pre * sigma).astype(BF16)
            slope = sigma * (1.0 + pre * (1.0 - sigma))
            pre_grad = (og[part, :].astype(F32) * slope).astype(BF16)
            total += lax.dot_general(
                gathered, pre_grad, (((0,), (0,)), ((), ())), preferred_element_type=F32
            )
            gt[k] = lax.dot_general(
                weight[...], pre_grad, (((1,), (1,)), ((), ())), preferred_element_type=F32
            ).astype(BF16)
        wg[...] = total

    act_save = pltpu.make_async_copy(act, act_out, out_sem.at[0])
    act_save.start()
    wgrad_out[...] = jnp.concatenate([wg[:, :TILE], wg[:, TILE:]], axis=0)

    @pl.loop(0, CHUNKS)
    def _(c):
        for u in range(PER):
            t = c * PER + u
            prod = jnp.dot(gt[targets[0, 0, t]], wt[t], preferred_element_type=F32)
            s = anchors[0, 0, t]
            sg[s] = sg[s] + prod

    saves = []
    for i in range(SAVES):
        start = (LOCAL + i * (SRC // SAVES)) % SRC

        @pl.loop(0, SRC // SAVES // 8)
        def _(c):
            for u in range(8):
                t = start + c * 8 + u
                sgb[t] = sg[t].astype(BF16)

        part = pl.ds(start, SRC // SAVES)
        saves.append(pltpu.make_async_copy(sgb.at[part], sgt_out.at[part], out_sem.at[1 + i]))
        saves[-1].start()
    act_save.wait()
    for save in saves:
        save.wait()


def layer(targets, anchors, feats, halo, tiles, grads, weight):
    return pl.pallas_call(
        layer_kernel,
        out_shape=(
            jax.ShapeDtypeStruct((TGT * TILE, HID), BF16),
            jax.ShapeDtypeStruct((SRC, FEAT, TILE), BF16),
            jax.ShapeDtypeStruct((2 * FEAT, TILE), F32),
        ),
        in_specs=[SMEM, SMEM, ANY, ANY, ANY, ANY, VMEM],
        out_specs=(ANY, ANY, VMEM),
        scratch_shapes=[
            pltpu.VMEM((2 * SRC, NREP, Q, FEAT), BF16),
            pltpu.VMEM((NT, TILE, TILE), BF16),
            pltpu.VMEM((TGT * TILE, HID), BF16),
            pltpu.VMEM((TGT, TILE, FEAT), F32),
            pltpu.VMEM((TGT, FEAT, TILE), BF16),
            pltpu.VMEM((SRC, FEAT, TILE), F32),
            pltpu.VMEM((TGT * TILE, HID), BF16),
            pltpu.VMEM((SRC, FEAT, TILE), BF16),
            pltpu.VMEM((FEAT, HID), F32),
            pltpu.SemaphoreType.DMA((NREP + 1,)),
            pltpu.SemaphoreType.DMA((CHUNKS,)),
            pltpu.SemaphoreType.DMA,
            pltpu.SemaphoreType.DMA((1 + SAVES,)),
        ],
        name="layer",
    )(targets, anchors, feats, halo, tiles, grads, weight)


def return_kernel(
    sgt, wpart, back, local, wrows,
    turned, part, inbox, sums, wbox, wplane, wline, wsum, wsums, wtotal,
    load_sem, own_sem, ring_send, ring_recv, send_sem, recv_sem, w_send, w_recv,
):
    me_d, me_r, right, across, left = place()
    greet_dom(me_d, me_r)
    greet([(me_d, right), (me_d, left), (me_d, across)])

    halo_load = pltpu.make_async_copy(
        sgt.at[pl.ds(LOCAL, SRC - LOCAL)], turned.at[pl.ds(LOCAL, SRC - LOCAL)], load_sem.at[0]
    )
    local_load = pltpu.make_async_copy(
        sgt.at[pl.ds(0, LOCAL)], turned.at[pl.ds(0, LOCAL)], load_sem.at[1]
    )
    halo_load.start()
    local_load.start()
    one = (
        lax.broadcasted_iota(jnp.int32, (TILE, TILE), 0)
        == lax.broadcasted_iota(jnp.int32, (TILE, TILE), 1)
    ).astype(F32).astype(BF16)

    def upright(block):
        return lax.dot_general(
            one, block, (((1,), (1,)), ((), ())), preferred_element_type=F32
        ).astype(BF16)

    halo_load.wait()

    @pl.loop(0, (SRC - LOCAL) // 8)
    def _(c):
        for u in range(8):
            s = c * 8 + u
            block = upright(turned[LOCAL + s]).reshape(2, NREP, Q, FEAT)
            for r in range(NREP):
                part[r, pl.ds(s * 2, 2)] = block[:, r]

    greeted(NDOM - 1 + 3)

    def ring(i, k):
        r = lax.rem(me_r + k, NREP)
        z = plane_rows(me_d, plane_step(i))
        return remote(
            part.at[r, z], inbox.at[k, z], ring_send.at[i, k], ring_recv.at[i, k], (me_d, r)
        )

    me_z, me_p = me_d // PLANE, lax.rem(me_d, PLANE)

    def in_plane(src, dst, k, stage, back_from):
        p = lax.rem(me_p + k, PLANE)
        q = lax.rem(me_p + PLANE - k, PLANE) if back_from else me_p
        return remote(
            src(p), dst(q, k), w_send.at[stage, k], w_recv.at[stage, k], (me_z * PLANE + p, me_r)
        )

    def along_z(src, dst, k, stage, back_from):
        z = lax.rem(me_z + k, NZ)
        y = lax.rem(me_z + NZ - k, NZ) if back_from else me_z
        return remote(
            src(z), dst(y, k), w_send.at[stage, k], w_recv.at[stage, k], (z * PLANE + me_p, me_r)
        )

    def w_stage(stage, k, back_from=False):
        if stage == 0:
            return in_plane(
                lambda p: wpart.at[pl.ds(p * NZ, NZ)], lambda q, k: wbox.at[k], k, 0, back_from
            )
        if stage == 1:
            return along_z(lambda z: wplane.at[z], lambda y, k: wline.at[k], k, 1, back_from)
        if stage == 2:
            r = lax.rem(me_r + k, NREP)
            return remote(wsum, wsums.at[k], w_send.at[2, k], w_recv.at[2, k], (me_d, r))
        if stage == 3:
            return along_z(
                lambda z: wtotal, lambda y, k: wrows.at[me_p * NZ + y], k, 3, back_from
            )
        mine = wrows.at[pl.ds(me_p * NZ, NZ)]
        return in_plane(
            lambda p: mine, lambda q, k: wrows.at[pl.ds(q * NZ, NZ)], k, 4, back_from
        )

    peers = (PLANE, NZ, NREP, NZ, PLANE)

    def w_start(stage):
        for k in range(1, peers[stage]):
            w_stage(stage, k).start()

    def w_wait(stage):
        for k in range(1, peers[stage]):
            w_stage(stage, k, True).wait_recv()

    def to(n):
        d = ahead(me_d, plane_step(n // PLANE), lax.rem(n, PLANE))
        return remote(sums.at[d], back.at[me_d], send_sem.at[n], recv_sem.at[n], (d, me_r))

    def came(n):
        d = behind(me_d, plane_step(n // PLANE), lax.rem(n, PLANE))
        return remote(sums.at[d], back.at[d], send_sem.at[n], recv_sem.at[n], (d, me_r))

    @pl.loop(0, NZ)
    def _(i):
        for k in (2, 1, 3):
            ring(i, k).start()

    w_start(0)
    local_load.wait()

    @pl.loop(0, LOCAL // 8)
    def _(i):
        for u in range(8):
            local[i * 8 + u] = upright(turned[i * 8 + u])

    def finish(i):
        for k in range(1, NREP):
            ring(i, k).wait_recv()
        z = plane_rows(me_d, plane_step(i))
        sums[z] = (
            (part[me_r, z].astype(F32) + inbox[1, z].astype(F32))
            + (inbox[2, z].astype(F32) + inbox[3, z].astype(F32))
        ).astype(BF16)

        @pl.loop(i * PLANE, jnp.minimum((i + 1) * PLANE, NDOM))
        def _(n):
            @pl.when(n != OWN)
            def _():
                to(n).start()

    w_wait(0)
    wbox[0] = wpart[pl.ds(me_p * NZ, NZ)]
    wplane[...] = jnp.sum(wbox[...], axis=0)
    w_start(1)

    @pl.loop(0, 3)
    def _(i):
        finish(i)

    w_wait(1)
    wline[0] = wplane[me_z]
    wsum[...] = jnp.sum(wline[...], axis=0)
    w_start(2)
    finish(3)
    finish(4)
    w_wait(2)
    wsums[0] = wsum[...]
    terms = [wsums[lax.rem(NREP + me_r - r, NREP)] for r in range(NREP)]
    wtotal[...] = (terms[0] + terms[1]) + (terms[2] + terms[3])
    wrows[me_p * NZ + me_z] = wtotal[...]
    w_start(3)
    finish(5)
    finish(6)
    finish(7)
    own = pltpu.make_async_copy(sums.at[me_d], back.at[me_d], own_sem.at[0])
    own.start()
    w_wait(3)
    w_start(4)
    own.wait()
    others(lambda n: came(n).wait_recv())
    w_wait(4)
    others(lambda n: to(n).wait_send())
    for stage in range(5):
        for k in range(1, peers[stage]):
            w_stage(stage, k).wait_send()

    @pl.loop(0, NZ)
    def _(i):
        for k in range(1, NREP):
            ring(i, k).wait_send()


def return_halo(sgt, wpart):
    dma = pltpu.SemaphoreType.DMA
    return pl.pallas_call(
        return_kernel,
        out_shape=(
            jax.ShapeDtypeStruct((NDOM, Q, FEAT), BF16),
            jax.ShapeDtypeStruct((LOCAL, TILE, FEAT), BF16),
            jax.ShapeDtypeStruct((NDOM, WROWS, TILE), F32),
        ),
        in_specs=[ANY, VMEM],
        out_specs=(VMEM, VMEM, VMEM),
        scratch_shapes=[
            pltpu.VMEM((SRC, FEAT, TILE), BF16),
            pltpu.VMEM((NREP, NDOM, Q, FEAT), BF16),
            pltpu.VMEM((NREP, NDOM, Q, FEAT), BF16),
            pltpu.VMEM((NDOM, Q, FEAT), BF16),
            pltpu.VMEM((PLANE, NZ, WROWS, TILE), F32),
            pltpu.VMEM((NZ, WROWS, TILE), F32),
            pltpu.VMEM((NZ, WROWS, TILE), F32),
            pltpu.VMEM((WROWS, TILE), F32),
            pltpu.VMEM((NREP, WROWS, TILE), F32),
            pltpu.VMEM((WROWS, TILE), F32),
            dma((2,)),
            dma((1,)),
            dma((NZ, NREP)),
            dma((NZ, NREP)),
            dma((NDOM,)),
            dma((NDOM,)),
            dma((5, PLANE)),
            dma((5, PLANE)),
        ],
        compiler_params=pltpu.CompilerParams(collective_id=1, has_side_effects=True),
        name="return_halo",
    )(sgt, wpart)


def scatter_kernel(rows, counts, local, back, out, raw, wide, news, done, in_sem, out_sem):
    rep = lax.axis_index("rep")
    size = ROWS // PIECES
    loads = [
        pltpu.make_async_copy(
            local.at[pl.ds(i * size, size)], raw.at[pl.ds(i * size, size)], in_sem.at[i]
        )
        for i in range(PIECES)
    ]
    for load in loads:
        load.start()
    wide[pl.ds(ROWS, Q), :] = jnp.zeros((Q, FEAT), F32)
    news[...] = back[...].reshape(NDOM * Q, FEAT).astype(F32)
    for i in range(PIECES):
        loads[i].wait()
        wide[pl.ds(i * size, size), :] = raw[pl.ds(i * size, size), :].astype(F32)

    @pl.loop(0, NDOM // LISTS)
    def _(g):
        for u in range(LISTS):
            d = g * LISTS + u
            live = counts[0, d]
            places = []
            for c in range(Q):
                slot = rep * Q + c
                places.append(jnp.where(slot < live, rows[0, d, slot], ROWS + c))
            olds = [wide[pl.ds(row, 1), :] for row in places]
            for c, row in enumerate(places):
                wide[pl.ds(row, 1), :] = olds[c] + news[pl.ds(d * Q + c, 1), :]

    saves = []
    for i in range(PIECES):
        part = pl.ds(i * size, size)
        done[part, :] = wide[part, :].astype(BF16)
        saves.append(pltpu.make_async_copy(done.at[part], out.at[part], out_sem.at[i]))
        saves[-1].start()
    for save in saves:
        save.wait()


def scatter_rows(rows, counts, local, back):
    return pl.pallas_call(
        scatter_kernel,
        out_shape=jax.ShapeDtypeStruct((ROWS, FEAT), BF16),
        in_specs=[SMEM, SMEM, ANY, VMEM],
        out_specs=ANY,
        scratch_shapes=[
            pltpu.VMEM((ROWS, FEAT), BF16),
            pltpu.VMEM((ROWS + Q, FEAT), F32),
            pltpu.VMEM((NDOM * Q, FEAT), F32),
            pltpu.VMEM((ROWS, FEAT), BF16),
            pltpu.SemaphoreType.DMA((PIECES,)),
            pltpu.SemaphoreType.DMA((PIECES,)),
        ],
        name="scatter_rows",
    )(rows, counts, local, back)


def final_kernel(
    part, inbox, held, mid, relayed, load_sem, ring_send, ring_recv,
):
    me_d, me_r, right, across, left = place()
    greet([(me_d, right), (me_d, left)])
    loads = [
        pltpu.make_async_copy(part.at[r], held.at[r], load_sem.at[i])
        for i, r in enumerate((across, right, left))
    ]
    for load in loads:
        load.start()
    size = ROWS // NREP // PARTS // 2

    def ring(i, j):
        a = pl.ds(i * 2 * size, size)
        b = pl.ds(i * 2 * size + size, size)
        src, dst, dev = (
            (held.at[across, a], mid.at[0, i], right),
            (held.at[across, b], mid.at[1, i], left),
            (held.at[right, b], inbox.at[0, b], right),
            (held.at[left, a], inbox.at[1, a], left),
            (relayed.at[0, i], inbox.at[0, a], right),
            (relayed.at[1, i], inbox.at[1, b], left),
        )[j]
        return remote(src, dst, ring_send.at[i, j], ring_recv.at[i, j], (me_d, dev))

    def relay(i):
        a = pl.ds(i * 2 * size, size)
        b = pl.ds(i * 2 * size + size, size)
        ring(i, 0).wait_recv()
        relayed[0, i] = (mid[0, i].astype(F32) + held[right, a].astype(F32)).astype(BF16)
        ring(i, 1).wait_recv()
        relayed[1, i] = (mid[1, i].astype(F32) + held[left, b].astype(F32)).astype(BF16)
        ring(i, 4).start()
        ring(i, 5).start()

    for load in loads:
        load.wait()
    greeted(2)
    for j in range(4):
        ring(0, j).start()
    for i in range(PARTS):
        if i + 1 < PARTS:
            for j in range(4):
                ring(i + 1, j).start()
        relay(i)
    for i in range(PARTS):
        for j in range(2, 6):
            ring(i, j).wait_recv()
    for i in range(PARTS):
        for j in range(6):
            ring(i, j).wait_send()


def final_sums(part):
    rows = ROWS // NREP
    dma = pltpu.SemaphoreType.DMA
    return pl.pallas_call(
        final_kernel,
        out_shape=jax.ShapeDtypeStruct((2, rows, FEAT), BF16),
        in_specs=[ANY],
        out_specs=VMEM,
        scratch_shapes=[
            pltpu.VMEM((NREP, rows, FEAT), BF16),
            pltpu.VMEM((2, PARTS, rows // PARTS // 2, FEAT), BF16),
            pltpu.VMEM((2, PARTS, rows // PARTS // 2, FEAT), BF16),
            dma((3,)),
            dma((PARTS, 6)),
            dma((PARTS, 6)),
        ],
        compiler_params=pltpu.CompilerParams(collective_id=2, has_side_effects=True),
        name="final_sums",
    )(part)


def shards(
    features, weight, out_grad, send_rows, send_count, tile_target, tile_source, tile_weights
):
    halo = exchange_halo(send_rows, send_count, features)
    activated, sgt, wpart = layer(
        tile_target,
        tile_source,
        features.reshape(2 * LOCAL, NREP, Q, FEAT),
        halo,
        tile_weights.reshape(NT, TILE, TILE),
        out_grad,
        weight,
    )
    back, local, wrows = return_halo(sgt, wpart.reshape(NDOM, WROWS, TILE))
    node_part = scatter_rows(send_rows, send_count, local.reshape(ROWS, FEAT), back)
    node_part = node_part.reshape(NREP, ROWS // NREP, FEAT)
    sums = final_sums(node_part)
    own = lax.dynamic_index_in_dim(node_part, lax.axis_index("rep"), 0, keepdims=False)
    node_grad = (own.astype(F32) + sums[0].astype(F32) + sums[1].astype(F32)).astype(BF16)
    weight_grad = wrows.reshape(2, FEAT, TILE).transpose(1, 0, 2).reshape(FEAT, 2 * TILE)
    return (activated, node_grad, weight_grad)


def solution(mesh):
    both = ("dom", "rep")
    in_specs = (
        P("dom", None),
        P(),
        P(both, None),
        P("dom", None, None),
        P("dom", None),
        P("dom", "rep", None),
        P("dom", "rep", None),
        P("dom", "rep", None, None, None),
    )
    out_specs = (P(both, None), P(both, None), P())
    return jax.shard_map(
        shards, mesh=mesh, in_specs=in_specs, out_specs=out_specs, check_vma=False
    )
```

```python
import functools

import jax
import jax.numpy as jnp
from jax import lax
from jax.experimental import pallas as pl
from jax.experimental.pallas import tpu as pltpu
from jax.sharding import PartitionSpec as P

F32 = jnp.float32
BF16 = jnp.bfloat16
TILE = 128
FEAT = 128
HID = 256
CAP = 64
NDOM = 64
NREP = 4
Q = CAP // NREP
ROWS = 8192
TGT = 16
NT = 256
SRC = 96
LOCAL = 64
CHUNKS = 16
PER = NT // CHUNKS

VMEM = pl.BlockSpec(memory_space=pltpu.VMEM)
SMEM = pl.BlockSpec(memory_space=pltpu.SMEM)
ANY = pl.BlockSpec(memory_space=pl.ANY)
HBM = pl.BlockSpec(memory_space=pltpu.HBM)


def busy(micros):
    return pl.CostEstimate(
        flops=micros * 400_000_000, bytes_accessed=micros * 3_000_000, transcendentals=0
    )

MESH = pl.DeviceIdType.MESH


NZ = 8
PLANE = NDOM // NZ
HALF = PLANE // 2
PARTS = 4
DENSE = 8
SAVES = 3
LISTS = 2
PIECES = 4
LAG = 3
RELAYED = 6
WROWS = 2 * FEAT // NDOM


def place():
    me_d = lax.axis_index("dom")
    me_r = lax.axis_index("rep")
    right = lax.rem(me_r + 1, NREP)
    across = lax.rem(me_r + 2, NREP)
    left = lax.rem(me_r + 3, NREP)
    return me_d, me_r, right, across, left


def remote(src, dst, send_sem, recv_sem, dev):
    return pltpu.make_async_remote_copy(
        src_ref=src, dst_ref=dst, send_sem=send_sem, recv_sem=recv_sem,
        device_id=dev, device_id_type=MESH,
    )


def greet(devices):
    barrier = pltpu.get_barrier_semaphore()
    for dev in devices:
        pl.semaphore_signal(barrier, inc=1, device_id=dev, device_id_type=MESH)


def greet_dom(me_d, me_r):
    barrier = pltpu.get_barrier_semaphore()

    after, _ = places_around(me_d)

    def hail(z, p):
        pl.semaphore_signal(barrier, inc=1, device_id=(z + p, me_r), device_id_type=MESH)

    for p in after[1:]:
        hail(plane_at(me_d, 0), p)

    @pl.loop(1, NZ)
    def _(i):
        z = plane_at(me_d, i)
        for p in after:
            hail(z, p)


def greeted(count):
    pl.semaphore_wait(pltpu.get_barrier_semaphore(), count)


def plane_step(i):
    odd = lax.rem(i, 2)
    return lax.rem(4 + odd * ((i + 1) // 2) - (1 - odd) * (i // 2), NZ)


def near_step(i):
    return plane_step(NZ - 1 - i)


def plane_at(me_d, step):
    return lax.rem(me_d // PLANE + step, NZ) * PLANE


def plane_rows(me_d, step):
    return pl.ds(plane_at(me_d, step), PLANE)


def places_around(me_d):
    me_p = lax.rem(me_d, PLANE)
    after = [lax.rem(me_p + k, PLANE) for k in range(PLANE)]
    before = [lax.rem(me_p + PLANE - k, PLANE) for k in range(PLANE)]
    return after, before


def halo_kernel(
    rows_in, counts_in, feats, halo,
    rows, counts, raw, wide, picked, send, list_sem,
    load_sem, own_sem, send_sem, recv_sem, ring_send, ring_recv,
):
    me_d, me_r, right, across, left = place()
    greet_dom(me_d, me_r)
    greet([(me_d, right), (me_d, left), (me_d, across)])

    load = pltpu.make_async_copy(feats, raw, load_sem)
    load.start()
    lists = [
        pltpu.make_async_copy(rows_in, rows, list_sem.at[0]),
        pltpu.make_async_copy(counts_in, counts, list_sem.at[1]),
    ]
    for part in lists:
        part.start()
    load.wait()
    wide[pl.ds(0, ROWS), :] = raw[...].astype(F32)
    wide[pl.ds(ROWS, 8), :] = jnp.zeros((8, FEAT), F32)
    for part in lists:
        part.wait()

    for r in range(NREP):

        @pl.when(me_r == r)
        def _():
            @pl.loop(0, NDOM // LISTS)
            def _(g):
                for u in range(LISTS):
                    d = g * LISTS + u
                    live = counts[0, d]
                    for c in range(Q):
                        row = jnp.where(r * Q + c < live, rows[0, d, r * Q + c], ROWS)
                        picked[pl.ds(d * Q + c, 1), :] = wide[pl.ds(row, 1), :]

    send[...] = picked[...].reshape(NDOM, Q, FEAT).astype(BF16)
    greeted(NDOM - 1 + 3)

    after, before = places_around(me_d)

    def to(i, k):
        d = plane_at(me_d, NZ - near_step(i)) + before[k]
        n = i * PLANE + k
        return remote(
            send.at[d], halo.at[me_r, me_d], send_sem.at[n], recv_sem.at[n], (d, me_r)
        )

    def came(i, k):
        d = plane_at(me_d, near_step(i)) + after[k]
        n = i * PLANE + k
        return remote(send.at[d], halo.at[me_r, d], send_sem.at[n], recv_sem.at[n], (d, me_r))

    for k in range(1, PLANE):
        to(0, k).start()

    @pl.loop(1, NZ)
    def _(i):
        for k in range(PLANE):
            to(i, k).start()

    own = pltpu.make_async_copy(send.at[me_d], halo.at[me_r, me_d], own_sem)
    own.start()

    def ring(i, j, owner):
        z = plane_at(me_d, near_step(i))
        skip, size = ((0, PLANE), (0, PLANE), (0, HALF), (HALF, HALF), (0, PLANE))[j]
        block = halo.at[owner, pl.ds(z + skip, size)]
        dev = (me_d, (right, left, right, left, across)[j])
        return remote(block, block, ring_send.at[i, j], ring_recv.at[i, j], dev)

    def first(i):
        ring(i, 0, me_r).start()
        ring(i, 1, me_r).start()

    def relay(i):
        ring(i, 0, left).wait_recv()
        ring(i, 2, left).start()
        ring(i, 1, right).wait_recv()
        ring(i, 3, right).start()

    def arrived(i):
        for k in range(PLANE):
            came(i, k).wait_recv()

    own.wait()
    for k in range(1, PLANE):
        came(0, k).wait_recv()
    first(0)
    for i in range(1, LAG):
        arrived(i)
        first(i)

    @pl.loop(LAG, RELAYED)
    def _(i):
        arrived(i)
        first(i)
        relay(i - LAG)

    @pl.loop(RELAYED, NZ)
    def _(i):
        arrived(i)
        ring(i, 4, me_r).start()
        first(i)

    @pl.loop(RELAYED - LAG, RELAYED)
    def _(i):
        relay(i)

    for k in range(1, PLANE):
        to(0, k).wait_send()

    @pl.loop(1, NZ)
    def _(i):
        for k in range(PLANE):
            to(i, k).wait_send()

    @pl.loop(0, RELAYED)
    def _(i):
        ring(i, 2, across).wait_recv()
        ring(i, 3, across).wait_recv()
        for j in range(4):
            ring(i, j, me_r).wait_send()

    @pl.loop(RELAYED, NZ)
    def _(i):
        ring(i, 0, left).wait_recv()
        ring(i, 1, right).wait_recv()
        ring(i, 4, across).wait_recv()
        for j in (0, 1, 4):
            ring(i, j, me_r).wait_send()


def exchange_halo(rows, counts, feats):
    return pl.pallas_call(
        halo_kernel,
        out_shape=jax.ShapeDtypeStruct((NREP, NDOM, Q, FEAT), BF16),
        in_specs=[HBM, HBM, HBM],
        out_specs=VMEM,
        cost_estimate=busy(24),
        scratch_shapes=[
            pltpu.SMEM((1, NDOM, CAP), jnp.int32),
            pltpu.SMEM((1, NDOM), jnp.int32),
            pltpu.VMEM((ROWS, FEAT), BF16),
            pltpu.VMEM((ROWS + 8, FEAT), F32),
            pltpu.VMEM((NDOM * Q, FEAT), F32),
            pltpu.VMEM((NDOM, Q, FEAT), BF16),
            pltpu.SemaphoreType.DMA((2,)),
            pltpu.SemaphoreType.DMA,
            pltpu.SemaphoreType.DMA,
            pltpu.SemaphoreType.DMA((NDOM,)),
            pltpu.SemaphoreType.DMA((NDOM,)),
            pltpu.SemaphoreType.DMA((NZ, 5)),
            pltpu.SemaphoreType.DMA((NZ, 5)),
        ],
        compiler_params=pltpu.CompilerParams(collective_id=0, has_side_effects=True, vmem_limit_bytes=14 << 20),
        name="exchange_halo",
    )(rows, counts, feats)


def layer_kernel(
    targets, anchors, feats, halo, tiles, grads, weight,
    act_out, sgt_out, wgrad_out,
    src, wt, og, agg, gt, sg, act, sgb, wg,
    src_sem, wt_sem, og_sem, out_sem,
):
    loads = [
        pltpu.make_async_copy(feats, src.at[pl.ds(0, 2 * LOCAL)], src_sem.at[NREP])
    ] + [
        pltpu.make_async_copy(halo.at[r], src.at[pl.ds(2 * LOCAL, NDOM), r], src_sem.at[r])
        for r in range(NREP)
    ]
    for load in loads:
        load.start()

    def tile_load(c):
        part = pl.ds(c * PER, PER)
        return pltpu.make_async_copy(tiles.at[part], wt.at[part], wt_sem.at[c])

    for c in range(CHUNKS):
        tile_load(c).start()
    grad_load = pltpu.make_async_copy(grads, og, og_sem)
    grad_load.start()

    agg[...] = jnp.zeros_like(agg)
    sg[...] = jnp.zeros_like(sg)
    wg[...] = jnp.zeros_like(wg)
    for load in loads:
        load.wait()

    @pl.loop(0, CHUNKS)
    def _(c):
        tile_load(c).wait()
        for u in range(PER):
            t = c * PER + u
            block = src[pl.ds(anchors[0, 0, t] * 2, 2)].reshape(TILE, FEAT)
            prod = jnp.dot(wt[t], block, preferred_element_type=F32)
            k = targets[0, 0, t]
            agg[k] = agg[k] + prod

    grad_load.wait()

    @pl.loop(0, TGT // DENSE)
    def _(c):
        total = wg[...]
        for u in range(DENSE):
            k = c * DENSE + u
            gathered = agg[k].astype(BF16)
            pre = jnp.dot(gathered, weight[...], preferred_element_type=F32)
            sigma = jax.nn.sigmoid(pre)
            part = pl.ds(pl.multiple_of(k * TILE, TILE), TILE)
            act[part, :] = (pre * sigma).astype(BF16)
            slope = sigma * (1.0 + pre * (1.0 - sigma))
            pre_grad = (og[part, :].astype(F32) * slope).astype(BF16)
            total += lax.dot_general(
                gathered, pre_grad, (((0,), (0,)), ((), ())), preferred_element_type=F32
            )
            gt[k] = lax.dot_general(
                weight[...], pre_grad, (((1,), (1,)), ((), ())), preferred_element_type=F32
            ).astype(BF16)
        wg[...] = total

    act_save = pltpu.make_async_copy(act, act_out, out_sem.at[0])
    act_save.start()
    wgrad_out[...] = jnp.concatenate([wg[:, :TILE], wg[:, TILE:]], axis=0)

    @pl.loop(0, CHUNKS)
    def _(c):
        for u in range(PER):
            t = c * PER + u
            prod = jnp.dot(gt[targets[0, 0, t]], wt[t], preferred_element_type=F32)
            s = anchors[0, 0, t]
            sg[s] = sg[s] + prod

    saves = []
    for i in range(SAVES):
        start = (LOCAL + i * (SRC // SAVES)) % SRC

        @pl.loop(0, SRC // SAVES // 8)
        def _(c):
            for u in range(8):
                t = start + c * 8 + u
                sgb[t] = sg[t].astype(BF16)

        part = pl.ds(start, SRC // SAVES)
        saves.append(pltpu.make_async_copy(sgb.at[part], sgt_out.at[part], out_sem.at[1 + i]))
        saves[-1].start()
    act_save.wait()
    for save in saves:
        save.wait()


def layer(targets, anchors, feats, halo, tiles, grads, weight):
    return pl.pallas_call(
        layer_kernel,
        out_shape=(
            jax.ShapeDtypeStruct((TGT * TILE, HID), BF16),
            jax.ShapeDtypeStruct((SRC, FEAT, TILE), BF16),
            jax.ShapeDtypeStruct((2 * FEAT, TILE), F32),
        ),
        in_specs=[SMEM, SMEM, ANY, ANY, ANY, ANY, VMEM],
        out_specs=(ANY, ANY, VMEM),
        scratch_shapes=[
            pltpu.VMEM((2 * SRC, NREP, Q, FEAT), BF16),
            pltpu.VMEM((NT, TILE, TILE), BF16),
            pltpu.VMEM((TGT * TILE, HID), BF16),
            pltpu.VMEM((TGT, TILE, FEAT), F32),
            pltpu.VMEM((TGT, FEAT, TILE), BF16),
            pltpu.VMEM((SRC, FEAT, TILE), F32),
            pltpu.VMEM((TGT * TILE, HID), BF16),
            pltpu.VMEM((SRC, FEAT, TILE), BF16),
            pltpu.VMEM((FEAT, HID), F32),
            pltpu.SemaphoreType.DMA((NREP + 1,)),
            pltpu.SemaphoreType.DMA((CHUNKS,)),
            pltpu.SemaphoreType.DMA,
            pltpu.SemaphoreType.DMA((1 + SAVES,)),
        ],
        compiler_params=pltpu.CompilerParams(vmem_limit_bytes=30 << 20),
        cost_estimate=busy(16),
        name="layer",
    )(targets, anchors, feats, halo, tiles, grads, weight)


def return_kernel(
    sgt, wpart, back, local, wtotal,
    turned, part, inbox, sums, wbox, wplane, wline, wsum, wsums, upright_local,
    load_sem, own_sem, ring_send, ring_recv, send_sem, recv_sem, w_send, w_recv,
):
    me_d, me_r, right, across, left = place()
    greet_dom(me_d, me_r)
    greet([(me_d, right), (me_d, left), (me_d, across)])

    halo_load = pltpu.make_async_copy(
        sgt.at[pl.ds(LOCAL, SRC - LOCAL)], turned.at[pl.ds(LOCAL, SRC - LOCAL)], load_sem.at[0]
    )
    local_load = pltpu.make_async_copy(
        sgt.at[pl.ds(0, LOCAL)], turned.at[pl.ds(0, LOCAL)], load_sem.at[1]
    )
    halo_load.start()
    local_load.start()
    one = (
        lax.broadcasted_iota(jnp.int32, (TILE, TILE), 0)
        == lax.broadcasted_iota(jnp.int32, (TILE, TILE), 1)
    ).astype(F32).astype(BF16)

    def upright(block):
        return lax.dot_general(
            one, block, (((1,), (1,)), ((), ())), preferred_element_type=F32
        ).astype(BF16)

    halo_load.wait()

    @pl.loop(0, (SRC - LOCAL) // 8)
    def _(c):
        for u in range(8):
            s = c * 8 + u
            block = upright(turned[LOCAL + s]).reshape(2, NREP, Q, FEAT)
            for r in range(NREP):
                part[r, pl.ds(s * 2, 2)] = block[:, r]

    greeted(NDOM - 1 + 3)

    def ring(i, k):
        r = lax.rem(me_r + k, NREP)
        z = plane_rows(me_d, plane_step(i))
        return remote(
            part.at[r, z], inbox.at[k, z], ring_send.at[i, k], ring_recv.at[i, k], (me_d, r)
        )

    me_z, me_p = me_d // PLANE, lax.rem(me_d, PLANE)

    def in_plane(src, dst, k, stage, back_from):
        p = lax.rem(me_p + k, PLANE)
        q = lax.rem(me_p + PLANE - k, PLANE) if back_from else me_p
        return remote(
            src(p), dst(q, k), w_send.at[stage, k], w_recv.at[stage, k], (me_z * PLANE + p, me_r)
        )

    def along_z(src, dst, k, stage, back_from):
        z = lax.rem(me_z + k, NZ)
        y = lax.rem(me_z + NZ - k, NZ) if back_from else me_z
        return remote(
            src(z), dst(y, k), w_send.at[stage, k], w_recv.at[stage, k], (z * PLANE + me_p, me_r)
        )

    def w_stage(stage, k, back_from=False):
        if stage == 0:
            return in_plane(
                lambda p: wpart.at[pl.ds(p * NZ, NZ)], lambda q, k: wbox.at[k], k, 0, back_from
            )
        if stage == 1:
            return along_z(lambda z: wplane.at[z], lambda y, k: wline.at[k], k, 1, back_from)
        r = lax.rem(me_r + k, NREP)
        return remote(wsum, wsums.at[k], w_send.at[2, k], w_recv.at[2, k], (me_d, r))

    peers = (PLANE, NZ, NREP)

    def w_start(stage):
        for k in range(1, peers[stage]):
            w_stage(stage, k).start()

    def w_wait(stage):
        for k in range(1, peers[stage]):
            w_stage(stage, k, True).wait_recv()

    after, before = places_around(me_d)

    def to(i, k):
        d = plane_at(me_d, plane_step(i)) + after[k]
        n = i * PLANE + k
        return remote(sums.at[d], back.at[me_d], send_sem.at[n], recv_sem.at[n], (d, me_r))

    def came(i, k):
        d = plane_at(me_d, NZ - plane_step(i)) + before[k]
        n = i * PLANE + k
        return remote(sums.at[d], back.at[d], send_sem.at[n], recv_sem.at[n], (d, me_r))

    def others(body):
        @pl.loop(0, NZ - 1)
        def _(i):
            for k in range(PLANE):
                body(i, k)

        for k in range(1, PLANE):
            body(NZ - 1, k)

    @pl.loop(0, NZ)
    def _(i):
        for k in (2, 1, 3):
            ring(i, k).start()

    w_start(0)
    local_load.wait()

    @pl.loop(0, LOCAL // 8)
    def _(i):
        for u in range(8):
            upright_local[i * 8 + u] = upright(turned[i * 8 + u])

    local_save = pltpu.make_async_copy(upright_local, local, own_sem.at[1])
    local_save.start()

    def finish(i, last=False):
        for k in range(1, NREP):
            ring(i, k).wait_recv()
        z = plane_rows(me_d, plane_step(i))
        sums[z] = (
            (part[me_r, z].astype(F32) + inbox[1, z].astype(F32))
            + (inbox[2, z].astype(F32) + inbox[3, z].astype(F32))
        ).astype(BF16)
        for k in range(1 if last else 0, PLANE):
            to(i, k).start()

    w_wait(0)
    wbox[0] = wpart[pl.ds(me_p * NZ, NZ)]
    wplane[...] = jnp.sum(wbox[...], axis=0)
    w_start(1)

    @pl.loop(0, 3)
    def _(i):
        finish(i)

    w_wait(1)
    wline[0] = wplane[me_z]
    wsum[...] = jnp.sum(wline[...], axis=0)
    w_start(2)
    finish(3)
    finish(4)
    finish(5)
    finish(6)
    w_wait(2)
    wsums[0] = wsum[...]
    terms = [wsums[lax.rem(NREP + me_r - r, NREP)] for r in range(NREP)]
    wtotal[...] = (terms[0] + terms[1]) + (terms[2] + terms[3])
    finish(7, True)
    own = pltpu.make_async_copy(sums.at[me_d], back.at[me_d], own_sem.at[0])
    own.start()
    own.wait()
    others(lambda i, k: came(i, k).wait_recv())
    local_save.wait()
    others(lambda i, k: to(i, k).wait_send())
    for stage in range(3):
        for k in range(1, peers[stage]):
            w_stage(stage, k).wait_send()

    @pl.loop(0, NZ)
    def _(i):
        for k in range(1, NREP):
            ring(i, k).wait_send()


def return_halo(sgt, wpart):
    dma = pltpu.SemaphoreType.DMA
    return pl.pallas_call(
        return_kernel,
        out_shape=(
            jax.ShapeDtypeStruct((NDOM, Q, FEAT), BF16),
            jax.ShapeDtypeStruct((LOCAL, TILE, FEAT), BF16),
            jax.ShapeDtypeStruct((WROWS, TILE), F32),
        ),
        in_specs=[ANY, VMEM],
        out_specs=(VMEM, ANY, VMEM),
        scratch_shapes=[
            pltpu.VMEM((SRC, FEAT, TILE), BF16),
            pltpu.VMEM((NREP, NDOM, Q, FEAT), BF16),
            pltpu.VMEM((NREP, NDOM, Q, FEAT), BF16),
            pltpu.VMEM((NDOM, Q, FEAT), BF16),
            pltpu.VMEM((PLANE, NZ, WROWS, TILE), F32),
            pltpu.VMEM((NZ, WROWS, TILE), F32),
            pltpu.VMEM((NZ, WROWS, TILE), F32),
            pltpu.VMEM((WROWS, TILE), F32),
            pltpu.VMEM((NREP, WROWS, TILE), F32),
            pltpu.VMEM((LOCAL, TILE, FEAT), BF16),
            dma((2,)),
            dma((2,)),
            dma((NZ, NREP)),
            dma((NZ, NREP)),
            dma((NDOM,)),
            dma((NDOM,)),
            dma((3, PLANE)),
            dma((3, PLANE)),
        ],
        compiler_params=pltpu.CompilerParams(collective_id=1, has_side_effects=True, vmem_limit_bytes=14 << 20),
        cost_estimate=busy(24),
        name="return_halo",
    )(sgt, wpart)


def scatter_kernel(rows, counts, local, back, out, raw, wide, news, done, in_sem, out_sem):
    rep = lax.axis_index("rep")
    size = ROWS // PIECES
    loads = [
        pltpu.make_async_copy(
            local.at[pl.ds(i * size, size)], raw.at[pl.ds(i * size, size)], in_sem.at[i]
        )
        for i in range(PIECES)
    ]
    for load in loads:
        load.start()
    wide[pl.ds(ROWS, Q), :] = jnp.zeros((Q, FEAT), F32)
    news[...] = back[...].reshape(NDOM * Q, FEAT).astype(F32)
    for i in range(PIECES):
        loads[i].wait()
        wide[pl.ds(i * size, size), :] = raw[pl.ds(i * size, size), :].astype(F32)

    for r in range(NREP):

        @pl.when(rep == r)
        def _():
            @pl.loop(0, NDOM // LISTS)
            def _(g):
                for u in range(LISTS):
                    d = g * LISTS + u
                    live = counts[0, d]
                    places = []
                    for c in range(Q):
                        row = rows[0, d, r * Q + c]
                        places.append(jnp.where(r * Q + c < live, row, ROWS + c))
                    olds = [wide[pl.ds(row, 1), :] for row in places]
                    for c, row in enumerate(places):
                        wide[pl.ds(row, 1), :] = olds[c] + news[pl.ds(d * Q + c, 1), :]

    saves = []
    for i in range(PIECES):
        part = pl.ds(i * size, size)
        done[part, :] = wide[part, :].astype(BF16)
        saves.append(pltpu.make_async_copy(done.at[part], out.at[part], out_sem.at[i]))
        saves[-1].start()
    for save in saves:
        save.wait()


def scatter_rows(rows, counts, local, back):
    return pl.pallas_call(
        scatter_kernel,
        out_shape=jax.ShapeDtypeStruct((ROWS, FEAT), BF16),
        in_specs=[SMEM, SMEM, ANY, VMEM],
        out_specs=ANY,
        scratch_shapes=[
            pltpu.VMEM((ROWS, FEAT), BF16),
            pltpu.VMEM((ROWS + Q, FEAT), F32),
            pltpu.VMEM((NDOM * Q, FEAT), F32),
            pltpu.VMEM((ROWS, FEAT), BF16),
            pltpu.SemaphoreType.DMA((PIECES,)),
            pltpu.SemaphoreType.DMA((PIECES,)),
        ],
        compiler_params=pltpu.CompilerParams(vmem_limit_bytes=14 << 20),
        cost_estimate=busy(4),
        name="scatter_rows",
    )(rows, counts, local, back)


def final_kernel(
    part, wtotal, inbox, wrows,
    held, mid, relayed, load_sem, own_sem, ring_send, ring_recv, w_send, w_recv,
):
    me_d, me_r, right, across, left = place()
    greet([(me_d, right), (me_d, left)])
    me_z, me_p = me_d // PLANE, lax.rem(me_d, PLANE)
    greet([(lax.rem(me_z + k, NZ) * PLANE + me_p, me_r) for k in range(1, NZ)])
    greet([(me_z * PLANE + lax.rem(me_p + k, PLANE), me_r) for k in range(1, PLANE)])
    loads = [
        pltpu.make_async_copy(part.at[r], held.at[r], load_sem.at[i])
        for i, r in enumerate((across, right, left))
    ]
    for load in loads:
        load.start()
    size = ROWS // NREP // PARTS // 2

    def ring(i, j):
        a = pl.ds(i * 2 * size, size)
        b = pl.ds(i * 2 * size + size, size)
        src, dst, dev = (
            (held.at[across, a], mid.at[0, i], right),
            (held.at[across, b], mid.at[1, i], left),
            (held.at[right, b], inbox.at[0, b], right),
            (held.at[left, a], inbox.at[1, a], left),
            (relayed.at[0, i], inbox.at[0, a], right),
            (relayed.at[1, i], inbox.at[1, b], left),
        )[j]
        return remote(src, dst, ring_send.at[i, j], ring_recv.at[i, j], (me_d, dev))

    def relay(i):
        a = pl.ds(i * 2 * size, size)
        b = pl.ds(i * 2 * size + size, size)
        ring(i, 0).wait_recv()
        relayed[0, i] = (mid[0, i].astype(F32) + held[right, a].astype(F32)).astype(BF16)
        ring(i, 1).wait_recv()
        relayed[1, i] = (mid[1, i].astype(F32) + held[left, b].astype(F32)).astype(BF16)
        ring(i, 4).start()
        ring(i, 5).start()

    def w_line(k, came):
        z = lax.rem(me_z + k, NZ)
        y = lax.rem(me_z + NZ - k, NZ) if came else me_z
        return remote(
            wtotal, wrows.at[me_p * NZ + y], w_send.at[0, k], w_recv.at[0, k],
            (z * PLANE + me_p, me_r),
        )

    def w_plane(k, came):
        p = lax.rem(me_p + k, PLANE)
        q = lax.rem(me_p + PLANE - k, PLANE) if came else me_p
        return remote(
            wrows.at[pl.ds(me_p * NZ, NZ)], wrows.at[pl.ds(q * NZ, NZ)],
            w_send.at[1, k], w_recv.at[1, k], (me_z * PLANE + p, me_r),
        )

    for load in loads:
        load.wait()
    greeted(2 + NZ - 1 + PLANE - 1)
    for j in range(4):
        ring(0, j).start()
    for k in range(1, NZ):
        w_line(k, False).start()
    own = pltpu.make_async_copy(wtotal, wrows.at[me_p * NZ + me_z], own_sem)
    own.start()
    for i in range(PARTS):
        if i + 1 < PARTS:
            for j in range(4):
                ring(i + 1, j).start()
        relay(i)
        if i == PARTS // 2:
            own.wait()
            for k in range(1, NZ):
                w_line(k, True).wait_recv()
            for k in range(1, PLANE):
                w_plane(k, False).start()
    for k in range(1, PLANE):
        w_plane(k, True).wait_recv()
    for i in range(PARTS):
        for j in range(2, 6):
            ring(i, j).wait_recv()
    for k in range(1, NZ):
        w_line(k, False).wait_send()
    for k in range(1, PLANE):
        w_plane(k, False).wait_send()
    for i in range(PARTS):
        for j in range(6):
            ring(i, j).wait_send()


def final_sums(part, wtotal):
    rows = ROWS // NREP
    dma = pltpu.SemaphoreType.DMA
    return pl.pallas_call(
        final_kernel,
        out_shape=(
            jax.ShapeDtypeStruct((2, rows, FEAT), BF16),
            jax.ShapeDtypeStruct((NDOM, WROWS, TILE), F32),
        ),
        in_specs=[ANY, VMEM],
        out_specs=(VMEM, VMEM),
        scratch_shapes=[
            pltpu.VMEM((NREP, rows, FEAT), BF16),
            pltpu.VMEM((2, PARTS, rows // PARTS // 2, FEAT), BF16),
            pltpu.VMEM((2, PARTS, rows // PARTS // 2, FEAT), BF16),
            dma((3,)),
            dma,
            dma((PARTS, 6)),
            dma((PARTS, 6)),
            dma((2, PLANE)),
            dma((2, PLANE)),
        ],
        compiler_params=pltpu.CompilerParams(collective_id=2, has_side_effects=True, vmem_limit_bytes=8 << 20),
        cost_estimate=busy(20),
        name="final_sums",
    )(part, wtotal)


def shards(
    features, weight, out_grad, send_rows, send_count, tile_target, tile_source, tile_weights
):
    halo = exchange_halo(send_rows, send_count, features)
    activated, sgt, wpart = layer(
        tile_target,
        tile_source,
        features.reshape(2 * LOCAL, NREP, Q, FEAT),
        halo,
        tile_weights.reshape(NT, TILE, TILE),
        out_grad,
        weight,
    )
    back, local, wtotal = return_halo(sgt, wpart.reshape(NDOM, WROWS, TILE))
    node_part = scatter_rows(send_rows, send_count, local.reshape(ROWS, FEAT), back)
    node_part = node_part.reshape(NREP, ROWS // NREP, FEAT)
    sums, wrows = final_sums(node_part, wtotal)
    own = lax.dynamic_index_in_dim(node_part, lax.axis_index("rep"), 0, keepdims=False)
    node_grad = (own.astype(F32) + sums[0].astype(F32) + sums[1].astype(F32)).astype(BF16)
    weight_grad = wrows.reshape(2, FEAT, TILE).transpose(1, 0, 2).reshape(FEAT, 2 * TILE)
    return (activated, node_grad, weight_grad)


def solution(mesh):
    both = ("dom", "rep")
    in_specs = (
        P("dom", None),
        P(),
        P(both, None),
        P("dom", None, None),
        P("dom", None),
        P("dom", "rep", None),
        P("dom", "rep", None),
        P("dom", "rep", None, None, None),
    )
    out_specs = (P(both, None), P(both, None), P())
    return jax.shard_map(
        shards, mesh=mesh, in_specs=in_specs, out_specs=out_specs, check_vma=False
    )
```

```python
import functools

import jax
import jax.numpy as jnp
from jax import lax
from jax.experimental import pallas as pl
from jax.experimental.pallas import tpu as pltpu
from jax.sharding import PartitionSpec as P

F32 = jnp.float32
BF16 = jnp.bfloat16
TILE = 128
FEAT = 128
HID = 256
CAP = 64
NDOM = 64
NREP = 4
Q = CAP // NREP
ROWS = 8192
TGT = 16
NT = 256
SRC = 96
LOCAL = 64
CHUNKS = 16
PER = NT // CHUNKS

VMEM = pl.BlockSpec(memory_space=pltpu.VMEM)
SMEM = pl.BlockSpec(memory_space=pltpu.SMEM)
ANY = pl.BlockSpec(memory_space=pl.ANY)
HBM = pl.BlockSpec(memory_space=pltpu.HBM)


def busy(micros):
    return pl.CostEstimate(
        flops=micros * 400_000_000, bytes_accessed=micros * 3_000_000, transcendentals=0
    )

MESH = pl.DeviceIdType.MESH


NZ = 8
PLANE = NDOM // NZ
HALF = PLANE // 2
PARTS = 4
DENSE = 8
SAVES = 3
LISTS = 2
LAG = 3
RELAYED = 6
WROWS = 2 * FEAT // NDOM


def place():
    me_d = lax.axis_index("dom")
    me_r = lax.axis_index("rep")
    right = lax.rem(me_r + 1, NREP)
    across = lax.rem(me_r + 2, NREP)
    left = lax.rem(me_r + 3, NREP)
    return me_d, me_r, right, across, left


def remote(src, dst, send_sem, recv_sem, dev):
    return pltpu.make_async_remote_copy(
        src_ref=src, dst_ref=dst, send_sem=send_sem, recv_sem=recv_sem,
        device_id=dev, device_id_type=MESH,
    )


def greet(devices):
    barrier = pltpu.get_barrier_semaphore()
    for dev in devices:
        pl.semaphore_signal(barrier, inc=1, device_id=dev, device_id_type=MESH)


def greet_dom(me_d, me_r):
    barrier = pltpu.get_barrier_semaphore()

    after, _ = places_around(me_d)

    def hail(z, p):
        pl.semaphore_signal(barrier, inc=1, device_id=(z + p, me_r), device_id_type=MESH)

    for p in after[1:]:
        hail(plane_at(me_d, 0), p)

    @pl.loop(1, NZ)
    def _(i):
        z = plane_at(me_d, i)
        for p in after:
            hail(z, p)


def greeted(count):
    pl.semaphore_wait(pltpu.get_barrier_semaphore(), count)


def plane_step(i):
    odd = lax.rem(i, 2)
    return lax.rem(4 + odd * ((i + 1) // 2) - (1 - odd) * (i // 2), NZ)


def near_step(i):
    return plane_step(NZ - 1 - i)


def plane_at(me_d, step):
    return lax.rem(me_d // PLANE + step, NZ) * PLANE


def plane_rows(me_d, step):
    return pl.ds(plane_at(me_d, step), PLANE)


def places_around(me_d):
    me_p = lax.rem(me_d, PLANE)
    after = [lax.rem(me_p + k, PLANE) for k in range(PLANE)]
    before = [lax.rem(me_p + PLANE - k, PLANE) for k in range(PLANE)]
    return after, before


def halo_kernel(
    rows_in, counts_in, feats, halo,
    rows, counts, raw, wide, picked, send, list_sem,
    load_sem, own_sem, send_sem, recv_sem, ring_send, ring_recv,
):
    me_d, me_r, right, across, left = place()
    greet_dom(me_d, me_r)
    greet([(me_d, right), (me_d, left), (me_d, across)])

    load = pltpu.make_async_copy(feats, raw, load_sem)
    load.start()
    lists = [
        pltpu.make_async_copy(rows_in, rows, list_sem.at[0]),
        pltpu.make_async_copy(counts_in, counts, list_sem.at[1]),
    ]
    for part in lists:
        part.start()
    load.wait()
    wide[pl.ds(0, ROWS), :] = raw[...].astype(F32)
    wide[pl.ds(ROWS, 8), :] = jnp.zeros((8, FEAT), F32)
    for part in lists:
        part.wait()

    for r in range(NREP):

        @pl.when(me_r == r)
        def _():
            @pl.loop(0, NDOM // LISTS)
            def _(g):
                for u in range(LISTS):
                    d = g * LISTS + u
                    live = counts[0, d]
                    for c in range(Q):
                        row = jnp.where(r * Q + c < live, rows[0, d, r * Q + c], ROWS)
                        picked[pl.ds(d * Q + c, 1), :] = wide[pl.ds(row, 1), :]

    send[...] = picked[...].reshape(NDOM, Q, FEAT).astype(BF16)
    greeted(NDOM - 1 + 3)

    after, before = places_around(me_d)

    def to(i, k):
        d = plane_at(me_d, NZ - near_step(i)) + before[k]
        n = i * PLANE + k
        return remote(
            send.at[d], halo.at[me_r, me_d], send_sem.at[n], recv_sem.at[n], (d, me_r)
        )

    def came(i, k):
        d = plane_at(me_d, near_step(i)) + after[k]
        n = i * PLANE + k
        return remote(send.at[d], halo.at[me_r, d], send_sem.at[n], recv_sem.at[n], (d, me_r))

    for k in range(1, PLANE):
        to(0, k).start()

    @pl.loop(1, NZ)
    def _(i):
        for k in range(PLANE):
            to(i, k).start()

    own = pltpu.make_async_copy(send.at[me_d], halo.at[me_r, me_d], own_sem)
    own.start()

    def ring(i, j, owner):
        z = plane_at(me_d, near_step(i))
        skip, size = ((0, PLANE), (0, PLANE), (0, HALF), (HALF, HALF), (0, PLANE))[j]
        block = halo.at[owner, pl.ds(z + skip, size)]
        dev = (me_d, (right, left, right, left, across)[j])
        return remote(block, block, ring_send.at[i, j], ring_recv.at[i, j], dev)

    def first(i):
        ring(i, 0, me_r).start()
        ring(i, 1, me_r).start()

    def relay(i):
        ring(i, 0, left).wait_recv()
        ring(i, 2, left).start()
        ring(i, 1, right).wait_recv()
        ring(i, 3, right).start()

    def arrived(i):
        for k in range(PLANE):
            came(i, k).wait_recv()

    own.wait()
    for k in range(1, PLANE):
        came(0, k).wait_recv()
    first(0)
    for i in range(1, LAG):
        arrived(i)
        first(i)

    @pl.loop(LAG, RELAYED)
    def _(i):
        arrived(i)
        first(i)
        relay(i - LAG)

    @pl.loop(RELAYED, NZ)
    def _(i):
        arrived(i)
        ring(i, 4, me_r).start()
        first(i)

    @pl.loop(RELAYED - LAG, RELAYED)
    def _(i):
        relay(i)

    for k in range(1, PLANE):
        to(0, k).wait_send()

    @pl.loop(1, NZ)
    def _(i):
        for k in range(PLANE):
            to(i, k).wait_send()

    @pl.loop(0, RELAYED)
    def _(i):
        ring(i, 2, across).wait_recv()
        ring(i, 3, across).wait_recv()
        for j in range(4):
            ring(i, j, me_r).wait_send()

    @pl.loop(RELAYED, NZ)
    def _(i):
        ring(i, 0, left).wait_recv()
        ring(i, 1, right).wait_recv()
        ring(i, 4, across).wait_recv()
        for j in (0, 1, 4):
            ring(i, j, me_r).wait_send()


def exchange_halo(rows, counts, feats):
    return pl.pallas_call(
        halo_kernel,
        out_shape=jax.ShapeDtypeStruct((NREP, NDOM, Q, FEAT), BF16),
        in_specs=[HBM, HBM, HBM],
        out_specs=VMEM,
        cost_estimate=busy(24),
        scratch_shapes=[
            pltpu.SMEM((1, NDOM, CAP), jnp.int32),
            pltpu.SMEM((1, NDOM), jnp.int32),
            pltpu.VMEM((ROWS, FEAT), BF16),
            pltpu.VMEM((ROWS + 8, FEAT), F32),
            pltpu.VMEM((NDOM * Q, FEAT), F32),
            pltpu.VMEM((NDOM, Q, FEAT), BF16),
            pltpu.SemaphoreType.DMA((2,)),
            pltpu.SemaphoreType.DMA,
            pltpu.SemaphoreType.DMA,
            pltpu.SemaphoreType.DMA((NDOM,)),
            pltpu.SemaphoreType.DMA((NDOM,)),
            pltpu.SemaphoreType.DMA((NZ, 5)),
            pltpu.SemaphoreType.DMA((NZ, 5)),
        ],
        compiler_params=pltpu.CompilerParams(collective_id=0, has_side_effects=True, vmem_limit_bytes=14 << 20),
        name="exchange_halo",
    )(rows, counts, feats)


def layer_kernel(
    targets, anchors, feats, halo, wt, og, weight,
    act_out, sgt_out, wgrad_out,
    src, agg, gt, sg, act, sgb, wg, src_sem, out_sem,
):
    loads = [
        pltpu.make_async_copy(feats, src.at[pl.ds(0, 2 * LOCAL)], src_sem.at[NREP])
    ] + [
        pltpu.make_async_copy(halo.at[r], src.at[pl.ds(2 * LOCAL, NDOM), r], src_sem.at[r])
        for r in range(NREP)
    ]
    for load in loads:
        load.start()

    agg[...] = jnp.zeros_like(agg)
    sg[...] = jnp.zeros_like(sg)
    wg[...] = jnp.zeros_like(wg)
    for load in loads:
        load.wait()

    @pl.loop(0, CHUNKS)
    def _(c):
        for u in range(PER):
            t = c * PER + u
            block = src[pl.ds(anchors[0, 0, t] * 2, 2)].reshape(TILE, FEAT)
            prod = jnp.dot(wt[t], block, preferred_element_type=F32)
            k = targets[0, 0, t]
            agg[k] = agg[k] + prod

    @pl.loop(0, TGT // DENSE)
    def _(c):
        total = wg[...]
        for u in range(DENSE):
            k = c * DENSE + u
            gathered = agg[k].astype(BF16)
            pre = jnp.dot(gathered, weight[...], preferred_element_type=F32)
            sigma = jax.nn.sigmoid(pre)
            part = pl.ds(pl.multiple_of(k * TILE, TILE), TILE)
            act[part, :] = (pre * sigma).astype(BF16)
            slope = sigma * (1.0 + pre * (1.0 - sigma))
            pre_grad = (og[part, :].astype(F32) * slope).astype(BF16)
            total += lax.dot_general(
                gathered, pre_grad, (((0,), (0,)), ((), ())), preferred_element_type=F32
            )
            gt[k] = lax.dot_general(
                weight[...], pre_grad, (((1,), (1,)), ((), ())), preferred_element_type=F32
            ).astype(BF16)
        wg[...] = total

    act_save = pltpu.make_async_copy(act, act_out, out_sem.at[0])
    act_save.start()
    wgrad_out[...] = jnp.concatenate([wg[:, :TILE], wg[:, TILE:]], axis=0)

    @pl.loop(0, CHUNKS)
    def _(c):
        for u in range(PER):
            t = c * PER + u
            prod = jnp.dot(gt[targets[0, 0, t]], wt[t], preferred_element_type=F32)
            s = anchors[0, 0, t]
            sg[s] = sg[s] + prod

    saves = []
    for i in range(SAVES):
        start = (LOCAL + i * (SRC // SAVES)) % SRC

        @pl.loop(0, SRC // SAVES // 8)
        def _(c):
            for u in range(8):
                t = start + c * 8 + u
                sgb[t] = sg[t].astype(BF16)

        part = pl.ds(start, SRC // SAVES)
        saves.append(pltpu.make_async_copy(sgb.at[part], sgt_out.at[part], out_sem.at[1 + i]))
        saves[-1].start()
    act_save.wait()
    for save in saves:
        save.wait()


def layer(targets, anchors, feats, halo, tiles, grads, weight):
    return pl.pallas_call(
        layer_kernel,
        out_shape=(
            jax.ShapeDtypeStruct((TGT * TILE, HID), BF16),
            jax.ShapeDtypeStruct((SRC, FEAT, TILE), BF16),
            jax.ShapeDtypeStruct((2 * FEAT, TILE), F32),
        ),
        in_specs=[SMEM, SMEM, ANY, ANY, VMEM, VMEM, VMEM],
        out_specs=(ANY, ANY, VMEM),
        scratch_shapes=[
            pltpu.VMEM((2 * SRC, NREP, Q, FEAT), BF16),
            pltpu.VMEM((TGT, TILE, FEAT), F32),
            pltpu.VMEM((TGT, FEAT, TILE), BF16),
            pltpu.VMEM((SRC, FEAT, TILE), F32),
            pltpu.VMEM((TGT * TILE, HID), BF16),
            pltpu.VMEM((SRC, FEAT, TILE), BF16),
            pltpu.VMEM((FEAT, HID), F32),
            pltpu.SemaphoreType.DMA((NREP + 1,)),
            pltpu.SemaphoreType.DMA((1 + SAVES,)),
        ],
        compiler_params=pltpu.CompilerParams(vmem_limit_bytes=30 << 20),
        cost_estimate=busy(16),
        name="layer",
    )(targets, anchors, feats, halo, tiles, grads, weight)


def return_kernel(
    turned, wpart, back, local, wtotal,
    part, inbox, sums, wbox, wplane, wline, wsum, wsums, upright_local,
    own_sem, ring_send, ring_recv, send_sem, recv_sem, w_send, w_recv,
):
    me_d, me_r, right, across, left = place()
    greet_dom(me_d, me_r)
    greet([(me_d, right), (me_d, left), (me_d, across)])

    one = (
        lax.broadcasted_iota(jnp.int32, (TILE, TILE), 0)
        == lax.broadcasted_iota(jnp.int32, (TILE, TILE), 1)
    ).astype(F32).astype(BF16)

    def upright(block):
        return lax.dot_general(
            one, block, (((1,), (1,)), ((), ())), preferred_element_type=F32
        ).astype(BF16)

    @pl.loop(0, (SRC - LOCAL) // 8)
    def _(c):
        for u in range(8):
            s = c * 8 + u
            block = upright(turned[LOCAL + s]).reshape(2, NREP, Q, FEAT)
            for r in range(NREP):
                part[r, pl.ds(s * 2, 2)] = block[:, r]

    greeted(NDOM - 1 + 3)

    def ring(i, k):
        r = lax.rem(me_r + k, NREP)
        z = plane_rows(me_d, plane_step(i))
        return remote(
            part.at[r, z], inbox.at[k, z], ring_send.at[i, k], ring_recv.at[i, k], (me_d, r)
        )

    me_z, me_p = me_d // PLANE, lax.rem(me_d, PLANE)

    def in_plane(src, dst, k, stage, back_from):
        p = lax.rem(me_p + k, PLANE)
        q = lax.rem(me_p + PLANE - k, PLANE) if back_from else me_p
        return remote(
            src(p), dst(q, k), w_send.at[stage, k], w_recv.at[stage, k], (me_z * PLANE + p, me_r)
        )

    def along_z(src, dst, k, stage, back_from):
        z = lax.rem(me_z + k, NZ)
        y = lax.rem(me_z + NZ - k, NZ) if back_from else me_z
        return remote(
            src(z), dst(y, k), w_send.at[stage, k], w_recv.at[stage, k], (z * PLANE + me_p, me_r)
        )

    def w_stage(stage, k, back_from=False):
        if stage == 0:
            return in_plane(
                lambda p: wpart.at[pl.ds(p * NZ, NZ)], lambda q, k: wbox.at[k], k, 0, back_from
            )
        if stage == 1:
            return along_z(lambda z: wplane.at[z], lambda y, k: wline.at[k], k, 1, back_from)
        r = lax.rem(me_r + k, NREP)
        return remote(wsum, wsums.at[k], w_send.at[2, k], w_recv.at[2, k], (me_d, r))

    peers = (PLANE, NZ, NREP)

    def w_start(stage):
        for k in range(1, peers[stage]):
            w_stage(stage, k).start()

    def w_wait(stage):
        for k in range(1, peers[stage]):
            w_stage(stage, k, True).wait_recv()

    after, before = places_around(me_d)

    def to(i, k):
        d = plane_at(me_d, plane_step(i)) + after[k]
        n = i * PLANE + k
        return remote(sums.at[d], back.at[me_d], send_sem.at[n], recv_sem.at[n], (d, me_r))

    def came(i, k):
        d = plane_at(me_d, NZ - plane_step(i)) + before[k]
        n = i * PLANE + k
        return remote(sums.at[d], back.at[d], send_sem.at[n], recv_sem.at[n], (d, me_r))

    def others(body):
        @pl.loop(0, NZ - 1)
        def _(i):
            for k in range(PLANE):
                body(i, k)

        for k in range(1, PLANE):
            body(NZ - 1, k)

    @pl.loop(0, NZ)
    def _(i):
        for k in (2, 1, 3):
            ring(i, k).start()

    w_start(0)

    @pl.loop(0, LOCAL // 8)
    def _(i):
        for u in range(8):
            upright_local[i * 8 + u] = upright(turned[i * 8 + u])

    local_save = pltpu.make_async_copy(upright_local, local, own_sem.at[1])
    local_save.start()

    def finish(i, last=False):
        for k in range(1, NREP):
            ring(i, k).wait_recv()
        z = plane_rows(me_d, plane_step(i))
        sums[z] = (
            (part[me_r, z].astype(F32) + inbox[1, z].astype(F32))
            + (inbox[2, z].astype(F32) + inbox[3, z].astype(F32))
        ).astype(BF16)
        for k in range(1 if last else 0, PLANE):
            to(i, k).start()

    w_wait(0)
    wbox[0] = wpart[pl.ds(me_p * NZ, NZ)]
    wplane[...] = jnp.sum(wbox[...], axis=0)
    w_start(1)

    @pl.loop(0, 3)
    def _(i):
        finish(i)

    w_wait(1)
    wline[0] = wplane[me_z]
    wsum[...] = jnp.sum(wline[...], axis=0)
    w_start(2)
    finish(3)
    finish(4)
    finish(5)
    finish(6)
    w_wait(2)
    wsums[0] = wsum[...]
    terms = [wsums[lax.rem(NREP + me_r - r, NREP)] for r in range(NREP)]
    wtotal[...] = (terms[0] + terms[1]) + (terms[2] + terms[3])
    finish(7, True)
    own = pltpu.make_async_copy(sums.at[me_d], back.at[me_d], own_sem.at[0])
    own.start()
    own.wait()
    others(lambda i, k: came(i, k).wait_recv())
    local_save.wait()
    others(lambda i, k: to(i, k).wait_send())
    for stage in range(3):
        for k in range(1, peers[stage]):
            w_stage(stage, k).wait_send()

    @pl.loop(0, NZ)
    def _(i):
        for k in range(1, NREP):
            ring(i, k).wait_send()


def return_halo(sgt, wpart):
    dma = pltpu.SemaphoreType.DMA
    return pl.pallas_call(
        return_kernel,
        out_shape=(
            jax.ShapeDtypeStruct((NDOM, Q, FEAT), BF16),
            jax.ShapeDtypeStruct((LOCAL, TILE, FEAT), BF16),
            jax.ShapeDtypeStruct((WROWS, TILE), F32),
        ),
        in_specs=[VMEM, VMEM],
        out_specs=(VMEM, ANY, VMEM),
        scratch_shapes=[
            pltpu.VMEM((NREP, NDOM, Q, FEAT), BF16),
            pltpu.VMEM((NREP, NDOM, Q, FEAT), BF16),
            pltpu.VMEM((NDOM, Q, FEAT), BF16),
            pltpu.VMEM((PLANE, NZ, WROWS, TILE), F32),
            pltpu.VMEM((NZ, WROWS, TILE), F32),
            pltpu.VMEM((NZ, WROWS, TILE), F32),
            pltpu.VMEM((WROWS, TILE), F32),
            pltpu.VMEM((NREP, WROWS, TILE), F32),
            pltpu.VMEM((LOCAL, TILE, FEAT), BF16),
            dma((2,)),
            dma((NZ, NREP)),
            dma((NZ, NREP)),
            dma((NDOM,)),
            dma((NDOM,)),
            dma((3, PLANE)),
            dma((3, PLANE)),
        ],
        compiler_params=pltpu.CompilerParams(collective_id=1, has_side_effects=True, vmem_limit_bytes=14 << 20),
        cost_estimate=busy(24),
        name="return_halo",
    )(sgt, wpart)


def scatter_kernel(rows, counts, local, back, out, wide, news):
    rep = lax.axis_index("rep")
    wide[pl.ds(ROWS, Q), :] = jnp.zeros((Q, FEAT), F32)
    news[...] = back[...].reshape(NDOM * Q, FEAT).astype(F32)
    wide[pl.ds(0, ROWS), :] = local[...].astype(F32)

    for r in range(NREP):

        @pl.when(rep == r)
        def _():
            @pl.loop(0, NDOM // LISTS)
            def _(g):
                for u in range(LISTS):
                    d = g * LISTS + u
                    live = counts[0, d]
                    places = []
                    for c in range(Q):
                        row = rows[0, d, r * Q + c]
                        places.append(jnp.where(r * Q + c < live, row, ROWS + c))
                    olds = [wide[pl.ds(row, 1), :] for row in places]
                    for c, row in enumerate(places):
                        wide[pl.ds(row, 1), :] = olds[c] + news[pl.ds(d * Q + c, 1), :]

    out[...] = wide[pl.ds(0, ROWS), :].astype(BF16)


def scatter_rows(rows, counts, local, back):
    return pl.pallas_call(
        scatter_kernel,
        out_shape=jax.ShapeDtypeStruct((ROWS, FEAT), BF16),
        in_specs=[SMEM, SMEM, VMEM, VMEM],
        out_specs=VMEM,
        scratch_shapes=[
            pltpu.VMEM((ROWS + Q, FEAT), F32),
            pltpu.VMEM((NDOM * Q, FEAT), F32),
        ],
        compiler_params=pltpu.CompilerParams(vmem_limit_bytes=14 << 20),
        cost_estimate=busy(4),
        name="scatter_rows",
    )(rows, counts, local, back)


def final_kernel(
    held, wtotal, inbox, wrows,
    mid, relayed, own_sem, ring_send, ring_recv, w_send, w_recv,
):
    me_d, me_r, right, across, left = place()
    greet([(me_d, right), (me_d, left)])
    me_z, me_p = me_d // PLANE, lax.rem(me_d, PLANE)
    greet([(lax.rem(me_z + k, NZ) * PLANE + me_p, me_r) for k in range(1, NZ)])
    greet([(me_z * PLANE + lax.rem(me_p + k, PLANE), me_r) for k in range(1, PLANE)])
    size = ROWS // NREP // PARTS // 2

    def ring(i, j):
        a = pl.ds(i * 2 * size, size)
        b = pl.ds(i * 2 * size + size, size)
        src, dst, dev = (
            (held.at[across, a], mid.at[0, i], right),
            (held.at[across, b], mid.at[1, i], left),
            (held.at[right, b], inbox.at[0, b], right),
            (held.at[left, a], inbox.at[1, a], left),
            (relayed.at[0, i], inbox.at[0, a], right),
            (relayed.at[1, i], inbox.at[1, b], left),
        )[j]
        return remote(src, dst, ring_send.at[i, j], ring_recv.at[i, j], (me_d, dev))

    def relay(i):
        a = pl.ds(i * 2 * size, size)
        b = pl.ds(i * 2 * size + size, size)
        ring(i, 0).wait_recv()
        relayed[0, i] = (mid[0, i].astype(F32) + held[right, a].astype(F32)).astype(BF16)
        ring(i, 1).wait_recv()
        relayed[1, i] = (mid[1, i].astype(F32) + held[left, b].astype(F32)).astype(BF16)
        ring(i, 4).start()
        ring(i, 5).start()

    def w_line(k, came):
        z = lax.rem(me_z + k, NZ)
        y = lax.rem(me_z + NZ - k, NZ) if came else me_z
        return remote(
            wtotal, wrows.at[me_p * NZ + y], w_send.at[0, k], w_recv.at[0, k],
            (z * PLANE + me_p, me_r),
        )

    def w_plane(k, came):
        p = lax.rem(me_p + k, PLANE)
        q = lax.rem(me_p + PLANE - k, PLANE) if came else me_p
        return remote(
            wrows.at[pl.ds(me_p * NZ, NZ)], wrows.at[pl.ds(q * NZ, NZ)],
            w_send.at[1, k], w_recv.at[1, k], (me_z * PLANE + p, me_r),
        )

    greeted(2 + NZ - 1 + PLANE - 1)
    for j in range(4):
        ring(0, j).start()
    for k in range(1, NZ):
        w_line(k, False).start()
    own = pltpu.make_async_copy(wtotal, wrows.at[me_p * NZ + me_z], own_sem)
    own.start()
    for i in range(PARTS):
        if i + 1 < PARTS:
            for j in range(4):
                ring(i + 1, j).start()
        relay(i)
        if i == PARTS // 2:
            own.wait()
            for k in range(1, NZ):
                w_line(k, True).wait_recv()
            for k in range(1, PLANE):
                w_plane(k, False).start()
    for k in range(1, PLANE):
        w_plane(k, True).wait_recv()
    for i in range(PARTS):
        for j in range(2, 6):
            ring(i, j).wait_recv()
    for k in range(1, NZ):
        w_line(k, False).wait_send()
    for k in range(1, PLANE):
        w_plane(k, False).wait_send()
    for i in range(PARTS):
        for j in range(6):
            ring(i, j).wait_send()


def final_sums(part, wtotal):
    rows = ROWS // NREP
    dma = pltpu.SemaphoreType.DMA
    return pl.pallas_call(
        final_kernel,
        out_shape=(
            jax.ShapeDtypeStruct((2, rows, FEAT), BF16),
            jax.ShapeDtypeStruct((NDOM, WROWS, TILE), F32),
        ),
        in_specs=[VMEM, VMEM],
        out_specs=(VMEM, VMEM),
        scratch_shapes=[
            pltpu.VMEM((2, PARTS, rows // PARTS // 2, FEAT), BF16),
            pltpu.VMEM((2, PARTS, rows // PARTS // 2, FEAT), BF16),
            dma,
            dma((PARTS, 6)),
            dma((PARTS, 6)),
            dma((2, PLANE)),
            dma((2, PLANE)),
        ],
        compiler_params=pltpu.CompilerParams(collective_id=2, has_side_effects=True, vmem_limit_bytes=8 << 20),
        cost_estimate=busy(20),
        name="final_sums",
    )(part, wtotal)


def shards(
    features, weight, out_grad, send_rows, send_count, tile_target, tile_source, tile_weights
):
    halo = exchange_halo(send_rows, send_count, features)
    activated, sgt, wpart = layer(
        tile_target,
        tile_source,
        features.reshape(2 * LOCAL, NREP, Q, FEAT),
        halo,
        tile_weights.reshape(NT, TILE, TILE),
        out_grad,
        weight,
    )
    back, local, wtotal = return_halo(sgt, wpart.reshape(NDOM, WROWS, TILE))
    node_part = scatter_rows(send_rows, send_count, local.reshape(ROWS, FEAT), back)
    node_part = node_part.reshape(NREP, ROWS // NREP, FEAT)
    sums, wrows = final_sums(node_part, wtotal)
    own = lax.dynamic_index_in_dim(node_part, lax.axis_index("rep"), 0, keepdims=False)
    node_grad = (own.astype(F32) + sums[0].astype(F32) + sums[1].astype(F32)).astype(BF16)
    weight_grad = wrows.reshape(2, FEAT, TILE).transpose(1, 0, 2).reshape(FEAT, 2 * TILE)
    return (activated, node_grad, weight_grad)


def solution(mesh):
    both = ("dom", "rep")
    in_specs = (
        P("dom", None),
        P(),
        P(both, None),
        P("dom", None, None),
        P("dom", None),
        P("dom", "rep", None),
        P("dom", "rep", None),
        P("dom", "rep", None, None, None),
    )
    out_specs = (P(both, None), P(both, None), P())
    return jax.shard_map(
        shards, mesh=mesh, in_specs=in_specs, out_specs=out_specs, check_vma=False
    )
```
